256 devices in a mesh: gx: 16 (over x, z_lo), gy: 16 (over z_hi, y, core).
Axes of the slice: x: 4, y: 4, z: 8 (z_hi: 2, z_lo: 4; z = z_hi * 4 + z_lo), core: 2. Of those that a mesh axis runs over, the one named last changes fastest.
Arguments:
- right_side: float32 [3, 448, 49728], P(None, 'gx', 'gy'), may hold values from -6 to 6
- guess: float32 [3, 448, 49728], P(None, 'gx', 'gy'), may hold values from -6 to 6
- material: int32 [64, 64, 16], P('gx', 'gy'), may hold values from 0 to 7
- lame: float32 [2, 8], replicated, may hold values from 0.5 to 2
- upper: float32 [1], replicated, may hold values from 3 to 6
- lower_ratio: float32 [1], replicated, may hold values from 0.05 to 0.3
Outputs:
- smoothed: float32 [3, 448, 49728], P(None, 'gx', 'gy')
- residual: float32 [3, 448, 49728], P(None, 'gx', 'gy')
The draws below stay inside these ranges and needn't reach their ends.
All inputs are finite; a program needn't handle non-finite values.
Results may differ from the reference program's by a relative error of at most 0.0003.
Values sent between devices are 32-bit elements; how exact they have to be, the bound alone decides.
No kernel may reach another device: no remote copies, remote signals or barrier semaphores. Data moves between devices by JAX's collectives and lax.ppermute only.
A program may use at most 128 MiB of HBM per device.

```python
import math
import jax
import jax.numpy as jnp
import numpy as np
from jax import lax

DEG = 7
EZ = 16
NMAT = 8
SWEEPS = 2
CHEB = 3
NEX = 64
NEY = 64
NXN = 448
NYN = 448
ZN = 111


def plant(entries, rng, smallest, largest):
    dims = entries.shape
    place = [jax.random.randint(jax.random.fold_in(rng, axis), (), 0, dims[axis]) for axis in range(len(dims))]
    entries = entries.at[tuple(place)].set(smallest)
    longest = dims.index(max(dims))
    place[longest] = (place[longest] + 1) % dims[longest]
    return entries.at[tuple(place)].set(largest)


def block_levels(own_key, dims, split, low, largest):
    loudness = 1.0
    for axis_at, parts in split:
        heights = jax.random.uniform(jax.random.fold_in(jax.random.fold_in(own_key, 6), axis_at), (parts,), jnp.float32, low / len(split), largest / len(split))
        loudness = loudness * jnp.repeat(jnp.exp(heights), dims[axis_at] // parts).reshape((-1,) + (1,) * (len(dims) - 1 - axis_at))
    return loudness


def normal_values(own_key, shape, spread, most, cuts=(), kind=jnp.bfloat16):
    drawn = spread * jax.random.normal(own_key, shape, jnp.float32)
    if cuts:
        drawn = drawn * block_levels(own_key, shape, cuts, -0.22, 0.18)
    return jnp.clip(drawn, -most, most).astype(kind)


def setup_inputs(seed: int = 0) -> dict:
    seeds = jax.random.split(jax.random.key(seed), 7)
    return {
        "right_side": normal_values(seeds[0], (3, NXN, NYN * ZN), 0.5, 6.0, ((1, 16), (2, 16)), jnp.float32),
        "guess": normal_values(seeds[1], (3, NXN, NYN * ZN), 1.0, 6.0, ((1, 16), (2, 16)), jnp.float32),
        "material": plant(jax.random.randint(seeds[2], (NEX, NEY, EZ), 0, NMAT), jax.random.fold_in(seeds[2], 1), 0, NMAT - 1).astype(jnp.int32),
        "lame": jnp.clip(jnp.exp(jax.random.uniform(seeds[3], (2, NMAT), jnp.float32, math.log(0.5), math.log(2.0))), 0.5, 2.0),
        "upper": jnp.clip(jax.random.uniform(seeds[4], (1,), jnp.float32, 3.0, 6.0), 3.0, 6.0),
        "lower_ratio": jnp.clip(jax.random.uniform(seeds[5], (1,), jnp.float32, 0.05, 0.3), 0.05, 0.3),
    }


highest = lax.Precision.HIGHEST


def legendre_pair(points, degree):
    prev_poly = points * 0.0 + 1.0
    this_poly = points * 1.0
    for order in range(2, degree + 1):
        next_poly = ((2 * order - 1) * points * this_poly - (order - 1) * prev_poly) / order
        prev_poly = this_poly
        this_poly = next_poly
    return this_poly, prev_poly


def gll_tables(degree):
    count = degree + 1
    points = -np.cos(np.pi * np.arange(count) / degree)
    for newton_step in range(60):
        this_poly, prev_poly = legendre_pair(points, degree)
        points = points - (points * this_poly - prev_poly) / (count * this_poly)
    values, unused_poly = legendre_pair(points, degree)
    weights = 2.0 / (degree * (degree + 1) * values ** 2)
    identity_np = np.eye(count)
    spacing = points[:, None] - points[None, :] + identity_np
    derivative = values[:, None] / (values[None, :] * spacing) * (1.0 - identity_np)
    derivative[0, 0] = -degree * (degree + 1) / 4.0
    derivative[degree, degree] = degree * (degree + 1) / 4.0
    stiff_ratio = (weights[:, None] * derivative ** 2).sum(0) / weights
    return weights, derivative, stiff_ratio


def split_periodic(field_in, dim_index):
    layout = field_in.shape
    blocks = layout[dim_index] // DEG
    leading = field_in.reshape(layout[:dim_index] + (blocks, DEG) + layout[dim_index + 1:])
    first_node = lax.slice_in_dim(leading, 0, 1, axis=dim_index + 1)
    return jnp.concatenate([leading, jnp.roll(first_node, -1, axis=dim_index)], axis=dim_index + 1)


def fold_periodic(element_vals, dim_index):
    layout = element_vals.shape
    blocks = layout[dim_index]
    leading = lax.slice_in_dim(element_vals, 0, DEG, axis=dim_index + 1)
    trailing = lax.slice_in_dim(element_vals, DEG, DEG + 1, axis=dim_index + 1)
    first_node = lax.slice_in_dim(leading, 0, 1, axis=dim_index + 1) + jnp.roll(trailing, 1, axis=dim_index)
    remaining = lax.slice_in_dim(leading, 1, DEG, axis=dim_index + 1)
    joined = jnp.concatenate([first_node, remaining], axis=dim_index + 1)
    return joined.reshape(layout[:dim_index] + (blocks * DEG,) + layout[dim_index + 2:])


def split_clamped(field_in):
    layout = field_in.shape
    blocks = (layout[-1] + 1) // DEG
    widths = [(0, 0)] * (len(layout) - 1) + [(1, 1)]
    padded = jnp.pad(field_in, widths)
    leading = padded[..., :blocks * DEG].reshape(layout[:-1] + (blocks, DEG))
    trailing = padded[..., DEG::DEG][..., None]
    joined = jnp.concatenate([leading, trailing], -1)
    return joined.reshape(layout[:-1] + (blocks * (DEG + 1),))


def fold_clamped(element_vals):
    layout = element_vals.shape
    blocks = layout[-1] // (DEG + 1)
    split_vals = element_vals.reshape(layout[:-1] + (blocks, DEG + 1))
    leading = split_vals[..., :DEG].reshape(layout[:-1] + (blocks * DEG,))
    trailing = split_vals[..., DEG:]
    filler = jnp.zeros(layout[:-1] + (blocks, DEG - 1), element_vals.dtype)
    spread_tail = jnp.concatenate([filler, trailing], -1).reshape(layout[:-1] + (blocks * DEG,))
    no_pad = [(0, 0)] * (len(layout) - 1)
    full_line = jnp.pad(leading, no_pad + [(0, 1)]) + jnp.pad(spread_tail, no_pad + [(1, 0)])
    return full_line[..., 1:blocks * DEG]


def along_z(field_in, matrix):
    layout = field_in.shape
    split_vals = field_in.reshape(layout[:-1] + (layout[-1] // (DEG + 1), DEG + 1))
    return jnp.einsum('pk,...k->...p', matrix, split_vals, precision=highest).reshape(layout)


def element_forces(element_vals, lam_w, mu_w, derivative, z_grad, z_back):
    grad_x = jnp.einsum('pi,cxiyjz->cxpyjz', derivative, element_vals, precision=highest)
    grad_y = jnp.einsum('pj,cxiyjz->cxiypz', derivative, element_vals, precision=highest)
    grad_z = along_z(element_vals, z_grad)
    gradients = jnp.stack([grad_x, grad_y, grad_z])
    divergence = gradients[0, 0] + gradients[1, 1] + gradients[2, 2]
    identity = jnp.eye(3, dtype=jnp.float32).reshape(3, 3, 1, 1, 1, 1, 1)
    stress = mu_w * (gradients + jnp.swapaxes(gradients, 0, 1)) + lam_w * divergence * identity
    forces = jnp.einsum('pi,cxpyjz->cxiyjz', derivative, stress[0], precision=highest)
    forces = forces + jnp.einsum('pj,cxiypz->cxiyjz', derivative, stress[1], precision=highest)
    return forces + along_z(stress[2], z_back)


def element_diagonal(lam_w, mu_w, ratio_x, ratio_y, ratio_z):
    ratio_sum = ratio_x + ratio_y + ratio_z
    pieces = [lam_w * own_ratio + mu_w * (ratio_sum + own_ratio) for own_ratio in (ratio_x, ratio_y, ratio_z)]
    return jnp.stack(pieces)


def point_weight(weights, blocks_z):
    weights_z = jnp.tile(weights, blocks_z)
    return weights[None, :, None, None, None] * weights[None, None, None, :, None] * weights_z[None, None, None, None, :]


def point_coeffs(lam_el, mu_el, point_w):
    lam_rep = jnp.repeat(lam_el, DEG + 1, axis=2)[:, None, :, None, :]
    mu_rep = jnp.repeat(mu_el, DEG + 1, axis=2)[:, None, :, None, :]
    return lam_rep * point_w, mu_rep * point_w


def lame_fields(material, lame):
    labels = jnp.arange(lame.shape[1], dtype=jnp.int32)
    onehot = (material[..., None] == labels).astype(jnp.float32)
    coeffs = jnp.einsum('xyzm,km->kxyz', onehot, lame, precision=highest)
    return coeffs[0], coeffs[1]


def assemble_slabs(results):
    return fold_clamped(fold_periodic(jnp.moveaxis(results, 0, 1), 1))


def reference(right_side, guess, material, lame, upper, lower_ratio):
    weights_np, derivative_np, ratio_np = gll_tables(DEG)
    weights = jnp.asarray(weights_np, dtype=jnp.float32)
    derivative = jnp.asarray(derivative_np, dtype=jnp.float32)
    stiff_ratio = jnp.asarray(ratio_np, dtype=jnp.float32)
    point_w = point_weight(weights, EZ)
    ratio_x = stiff_ratio.reshape(1, DEG + 1, 1, 1, 1)
    ratio_y = stiff_ratio.reshape(1, 1, 1, DEG + 1, 1)
    ratio_z = jnp.tile(stiff_ratio, EZ).reshape(1, 1, 1, 1, -1)
    lam_el, mu_el = lame_fields(material, lame)
    shape_four = (3, NXN, NYN, ZN)
    source = right_side.reshape(shape_four)
    solution = guess.reshape(shape_four)

    def operate(field_in):
        slabs = jnp.moveaxis(split_periodic(split_clamped(field_in), 1), 1, 0)

        def one_slab(inputs):
            column_slab, lam_slab, mu_slab = inputs
            lam_w, mu_w = point_coeffs(lam_slab[None], mu_slab[None], point_w)
            element_vals = split_periodic(column_slab, 2)[:, None]
            forces = element_forces(element_vals, lam_w, mu_w, derivative, derivative, derivative.T)
            return fold_periodic(forces[:, 0], 2)

        return assemble_slabs(lax.map(one_slab, (slabs, lam_el, mu_el)))

    def diag_slab(inputs):
        lam_slab, mu_slab = inputs
        lam_w, mu_w = point_coeffs(lam_slab[None], mu_slab[None], point_w)
        pieces = element_diagonal(lam_w, mu_w, ratio_x, ratio_y, ratio_z)
        return fold_periodic(pieces[:, 0], 2)

    diagonal = assemble_slabs(lax.map(diag_slab, (lam_el, mu_el)))
    inverse = 1.0 / diagonal
    upper_edge = upper[0]
    lower_edge = lower_ratio[0] * upper_edge
    center = (upper_edge + lower_edge) / 2.0
    radius = (upper_edge - lower_edge) / 2.0
    sigma_ratio = center / radius
    for sweep_index in range(SWEEPS):
        residual = source - operate(solution)
        change = inverse * residual / center
        solution = solution + change
        factor = 1.0 / sigma_ratio
        for step_index in range(CHEB - 1):
            factor_next = 1.0 / (2.0 * sigma_ratio - factor)
            residual = source - operate(solution)
            change = factor_next * factor * change + (2.0 * factor_next / radius) * inverse * residual
            solution = solution + change
            factor = factor_next
    residual = source - operate(solution)
    flat_shape = (3, NXN, NYN * ZN)
    return solution.reshape(flat_shape), residual.reshape(flat_shape)
```

```python
import jax
import jax.numpy as jnp
import numpy as np
from jax import lax
from jax.experimental import pallas as pl
from jax.experimental.pallas import tpu as pltpu
from jax.sharding import PartitionSpec as P

DEG = 7
N = DEG + 1
SWEEPS = 2
CHEB = 3
F32 = jnp.float32
BF16 = jnp.bfloat16
highest = lax.Precision.HIGHEST


def legendre_pair(points, degree):
    prev_poly = points * 0.0 + 1.0
    this_poly = points * 1.0
    for order in range(2, degree + 1):
        next_poly = ((2 * order - 1) * points * this_poly - (order - 1) * prev_poly) / order
        prev_poly = this_poly
        this_poly = next_poly
    return (this_poly, prev_poly)


def gll_tables(degree):
    count = degree + 1
    points = -np.cos(np.pi * np.arange(count) / degree)
    for newton_step in range(60):
        this_poly, prev_poly = legendre_pair(points, degree)
        points = points - (points * this_poly - prev_poly) / (count * this_poly)
    values, unused_poly = legendre_pair(points, degree)
    weights = 2.0 / (degree * (degree + 1) * values**2)
    identity_np = np.eye(count)
    spacing = points[:, None] - points[None, :] + identity_np
    derivative = values[:, None] / (values[None, :] * spacing) * (1.0 - identity_np)
    derivative[0, 0] = -degree * (degree + 1) / 4.0
    derivative[degree, degree] = degree * (degree + 1) / 4.0
    stiff_ratio = (weights[:, None] * derivative**2).sum(0) / weights
    return (weights, derivative, stiff_ratio)


WEIGHTS, DERIV, RATIO = gll_tables(DEG)


def halves(matrix):
    high = matrix.astype(BF16).astype(np.float32)
    low = matrix.astype(np.float32) - high
    return high, low


def z_matrices(blocks):
    width = blocks * N
    node = np.array([DEG * f + k for f in range(blocks) for k in range(N)])
    free = (node > 0) & (node < DEG * blocks)
    share = ((node[:, None] == node[None, :]) & free[:, None] & free[None, :]).astype(np.float64)
    grad = np.kron(np.eye(blocks), DERIV.T)
    back = np.kron(np.eye(blocks), DERIV) @ share
    zero = np.zeros((width, width))
    grad_hi, grad_lo = halves(grad)
    back_hi, back_lo = halves(back)
    w_grad = np.block([[grad_hi, grad_lo], [grad_hi, zero]])
    w_back = np.block([[back_hi, back_lo], [back_hi, zero]])
    w_share = np.concatenate([share, share], 0)
    return w_grad, w_back, w_share


def line_sums(vals, matrix):
    even = [vals[i] + vals[DEG - i] for i in range(N // 2)]
    odd = [vals[i] - vals[DEG - i] for i in range(N // 2)]
    outs = [None] * N
    for p in range(N // 2):
        from_even = None
        from_odd = None
        for i in range(N // 2):
            ce = float(np.float32((matrix[p, i] + matrix[p, DEG - i]) / 2.0))
            co = float(np.float32((matrix[p, i] - matrix[p, DEG - i]) / 2.0))
            te = ce * even[i]
            to = co * odd[i]
            from_even = te if from_even is None else from_even + te
            from_odd = to if from_odd is None else from_odd + to
        outs[p] = from_odd + from_even
        outs[DEG - p] = from_odd - from_even
    return outs


def split_pair(value):
    high = value.astype(BF16)
    low = (value - high.astype(F32)).astype(BF16)
    return jnp.concatenate([high, low], axis=-1)


def dot(a, b):
    return jnp.dot(a, b, preferred_element_type=F32)


ROWS = 8
SIDE = 4
ORDER = (0, 3, 1, 2)
UNROLL = 2


def flip(value):
    return jnp.concatenate([value[SIDE:], value[:SIDE]], 0)


def received(par_ref, axis, even_ref, odd_ref, *at):
    is_even = par_ref[axis] == 0
    even = even_ref[at]
    odd = odd_ref[at]
    return jnp.where(is_even, even, odd), jnp.where(is_even, odd, even)


def sum_x(par_ref, xe_ref, xo_ref, parts, c, face_at, i, j, tile):
    total = parts[tile][c, i, j]
    if 0 < i < DEG:
        return total
    row = lax.broadcasted_iota(jnp.int32, (ROWS, 128), 0)
    across = DEG - i
    if tile == 0:
        right, left = received(par_ref, 0, xe_ref, xo_ref, face_at, j)
        face = right if i else left
        face = jnp.concatenate([face, face], 0)
        inner = parts[1][c, across, j]
        low, high = (inner, face) if i else (face, inner)
    else:
        middle = flip(parts[1][c, across, j])
        outer = parts[0][c, across, j]
        low, high = (middle, outer) if i else (outer, middle)
    return total + jnp.where(row < SIDE, low, high)


def sum_all(par_ref, faces, parts, c, face_at, i, j, tile, edge):
    xe, xo, ye, yo = faces
    total = sum_x(par_ref, xe, xo, parts, c, face_at, i, j, tile)
    if edge is not None:
        row = lax.broadcasted_iota(jnp.int32, (ROWS, 128), 0)
        top, bottom = received(par_ref, 1, ye, yo, face_at, i)
        face = top if edge else bottom
        at = SIDE - 1 if edge else 0
        first = jnp.broadcast_to(face[2 * tile : 2 * tile + 1], (ROWS, 128))
        second = jnp.broadcast_to(face[2 * tile + 1 : 2 * tile + 2], (ROWS, 128))
        total = total + jnp.where(row == at, first, jnp.where(row == SIDE + at, second, 0.0))
    return total


def over_planes(body):
    body(0, 0)

    def inner(j, carry):
        body(j, None)
        return carry

    lax.fori_loop(1, DEG, inner, 0, unroll=UNROLL)
    body(DEG, 1)


def loop(count, body, unroll=UNROLL):
    def inner(i, carry):
        body(i)
        return carry

    lax.fori_loop(0, count, inner, 0, unroll=unroll)


def gradients(planes, j, wg_ref, gx_ref, gz_ref):
    flat = jnp.concatenate([planes[c][i] for c in range(3) for i in range(N)], 0)
    both = dot(split_pair(flat), wg_ref[...])
    for c in range(3):
        outs = line_sums(planes[c], DERIV)
        for i in range(N):
            gx_ref[c, i, j] = outs[i]
    both = (both[:, :128] + both[:, 128:]).reshape(3, N, ROWS, 128)
    for c in range(3):
        for i in range(N):
            gz_ref[c, i, j] = both[c, i]


def finish(par_ref, u_ref, lam_ref, mu_ref, wb_ref, ws_ref, au_ref, gx_ref, gz_ref, fy_ref):
    def stress(i):
        gy = [line_sums([u_ref[c, i, j] for j in range(N)], DERIV) for c in range(3)]
        sy = [[None] * N for c in range(3)]
        sz = [[None] * N for c in range(3)]
        for j in range(N):
            gx = [gx_ref[c, i, j] for c in range(3)]
            gz = [gz_ref[c, i, j] for c in range(3)]
            mu = mu_ref[i, j]
            mu2 = mu + mu
            trace = lam_ref[i, j] * (gx[0] + gy[1][j] + gz[2])
            sxy = mu * (gx[1] + gy[0][j])
            sxz = mu * (gx[2] + gz[0])
            syz = mu * (gy[2][j] + gz[1])
            gx_ref[0, i, j] = mu2 * gx[0] + trace
            gx_ref[1, i, j] = sxy
            gx_ref[2, i, j] = sxz
            sz[0][j] = sxz
            sz[1][j] = syz
            sz[2][j] = mu2 * gz[2] + trace
            sy[0][j] = sxy
            sy[1][j] = mu2 * gy[1][j] + trace
            sy[2][j] = syz
        flat = jnp.concatenate([sz[c][j] for c in range(3) for j in range(N)], 0)
        both = dot(split_pair(flat), wb_ref[...])
        for c in range(3):
            outs = line_sums(sy[c], DERIV.T)
            for j in range(N):
                fy_ref[c, i, j] = outs[j]
        both = (both[:, :128] + both[:, 128:]).reshape(3, N, ROWS, 128)
        for c in range(3):
            gz_ref[c, i] = both[c]

    loop(N, stress)

    def back(j):
        flat = []
        for c in range(3):
            outs = line_sums([gx_ref[c, i, j] for i in range(N)], DERIV.T)
            flat += [outs[i] + fy_ref[c, i, j] for i in range(N)]
        both = dot(split_pair(jnp.concatenate(flat, 0)), ws_ref[...]).reshape(3, N, ROWS, 128)
        for c in range(3):
            for i in range(N):
                au_ref[c, i, j] = both[c, i] + gz_ref[c, i, j]

    loop(N, back)


def assemble(par_ref, part_ref, first, face_refs):
    row = lax.broadcasted_iota(jnp.int32, (ROWS, 128), 0)
    near = row % SIDE

    def along_y(i):
        for c in range(3):
            last = part_ref[c, i, DEG]
            start = part_ref[c, i, 0]
            last = last + jnp.where(near < SIDE - 1, jnp.concatenate([start[1:], start[:1]], 0), 0.0)
            start = jnp.where(near > 0, jnp.concatenate([last[-1:], last[:-1]], 0), start)
            part_ref[c, i, DEG] = last
            part_ref[c, i, 0] = start

    loop(N, along_y)
    if not face_refs:
        return
    xe_ref, xo_ref = face_refs
    is_even = par_ref[0] == 0

    def x_faces(j):
        for c in range(3):
            right = part_ref[c, DEG, j][SIDE:]
            left = part_ref[c, 0, j][:SIDE]
            xe_ref[first + c, j] = jnp.where(is_even, right, left)
            xo_ref[first + c, j] = jnp.where(is_even, left, right)

    loop(N, x_faces)


def first_kernel(tile, par_ref, ratio_ref, u_ref, lam_ref, mu_ref, rk_ref, wg_ref, wb_ref, ws_ref, au_ref, dg_ref, *refs):
    face_refs, work = refs[:-3], refs[-3:]
    gx_ref, gz_ref, fy_ref = work

    def diagonal(i):
        rows = [[None] * N for c in range(3)]
        for j in range(N):
            lam = lam_ref[i, j]
            mu = mu_ref[i, j]
            rk = rk_ref[...]
            total = rk + (ratio_ref[i] + float(RATIO[j]))
            for c in range(3):
                own = (ratio_ref[i], float(RATIO[j]), rk)[c]
                rows[c][j] = lam * own + mu * (total + own)
        flat = jnp.concatenate([rows[c][j] for c in range(3) for j in range(N)], 0)
        both = dot(split_pair(flat), ws_ref[...]).reshape(3, N, ROWS, 128)
        for c in range(3):
            dg_ref[c, i] = both[c]

    loop(N, diagonal)

    def start(j):
        planes = [[u_ref[c, i, j] for i in range(N)] for c in range(3)]
        gradients(planes, j, wg_ref, gx_ref, gz_ref)

    loop(N, start)
    finish(par_ref, u_ref, lam_ref, mu_ref, wb_ref, ws_ref, au_ref, gx_ref, gz_ref, fy_ref)
    assemble(par_ref, au_ref, 0, face_refs)
    assemble(par_ref, dg_ref, 3, face_refs)


def corner_kernel(par_ref, xe_ref, xo_ref, *refs):
    fields = [refs[k : k + 2] for k in range(0, len(refs) - 2, 2)]
    ye_ref, yo_ref = refs[-2:]
    is_even = par_ref[1] == 0
    for n, parts in enumerate(fields):
        for c in range(3):
            at = 3 * n + c
            for i in range(N):
                rows_t = []
                rows_b = []
                for tile in range(2):
                    top = sum_x(par_ref, xe_ref, xo_ref, parts, c, at, i, DEG, tile)
                    bottom = sum_x(par_ref, xe_ref, xo_ref, parts, c, at, i, 0, tile)
                    rows_t += [top[SIDE - 1 : SIDE], top[-1:]]
                    rows_b += [bottom[:1], bottom[SIDE : SIDE + 1]]
                top = jnp.concatenate(rows_t, 0)
                bottom = jnp.concatenate(rows_b, 0)
                ye_ref[at, i] = jnp.where(is_even, top, bottom)
                yo_ref[at, i] = jnp.where(is_even, bottom, top)


def step_kernel(tile, stage, with_diag, *refs):
    restart = stage == 0
    refs = list(refs)
    take = lambda count: [refs.pop(0) for _ in range(count)]
    par_ref, coef_ref, u_ref, b_ref = take(4)
    parts = take(2)
    faces = take(4)
    inv_refs = take(2 if with_diag else 1)
    change_ref = None if restart else refs.pop(0)
    lam_ref, mu_ref, wg_ref, wb_ref, ws_ref = take(5)
    u_out, change_out, au_ref = take(3)
    inv_out = refs.pop(0) if with_diag else None
    face_refs = take(2) if tile == 0 else []
    gx_ref, gz_ref, fy_ref = refs
    lane = lax.broadcasted_iota(jnp.int32, (ROWS, 128), 1)
    clamped = (lane == 0) | (lane == 127)

    def update(j, edge):
        keep = coef_ref[2 * stage]
        gain = coef_ref[2 * stage + 1]
        planes = [[None] * N for c in range(3)]
        for c in range(3):
            for i in range(N):
                if with_diag:
                    diag = sum_all(par_ref, faces, inv_refs, c, 3 + c, i, j, tile, edge)
                    inv = jnp.where(clamped, 0.0, 1.0 / jnp.where(clamped, 1.0, diag))
                    inv_out[c, i, j] = inv
                else:
                    inv = inv_refs[0][c, i, j]
                residual = b_ref[c, i, j] - sum_all(par_ref, faces, parts, c, c, i, j, tile, edge)
                change = gain * (inv * residual)
                if not restart:
                    change = keep * change_ref[c, i, j] + change
                change_out[c, i, j] = change
                planes[c][i] = u_ref[c, i, j] + change
                u_out[c, i, j] = planes[c][i]
        gradients(planes, j, wg_ref, gx_ref, gz_ref)

    over_planes(update)
    finish(par_ref, u_out, lam_ref, mu_ref, wb_ref, ws_ref, au_ref, gx_ref, gz_ref, fy_ref)
    assemble(par_ref, au_ref, 0, face_refs)


def last_kernel(par_ref, *refs):
    b_refs, parts, faces, res_refs = refs[:2], refs[2:4], refs[4:8], refs[8:]

    def update(j, edge):
        for tile in range(2):
            for c in range(3):
                for i in range(N):
                    total = sum_all(par_ref, faces, parts, c, c, i, j, tile, edge)
                    res_refs[tile][c, i, j] = b_refs[tile][c, i, j] - total

    over_planes(update)


def lane_pick(value, index):
    return jnp.take_along_axis(value, index, axis=1, mode="promise_in_bounds")


TILES = ((0, 8), (8, 16), (16, 24), (20, 28))


def load_kernel(par_ref, coef_ref, in_ref, t0_ref, t1_ref, xl_ref, yb_ref, work_ref):
    nodes_x, width = in_ref.shape[1], in_ref.shape[2]
    nodes_z = width // nodes_x
    outs = (t0_ref, t1_ref)
    lane = lax.broadcasted_iota(jnp.int32, (ROWS, 128), 1)
    node = DEG * (lane // N) + lane % N - 1
    free = (node >= 0) & (node < nodes_z)
    node = jnp.clip(node, 0, nodes_z - 1)
    zero = jnp.zeros((ROWS, 128), F32)
    for r in range(4):
        work_ref[nodes_x, pl.ds(8 * r, 8)] = zero

    def component(c, carry):
        for y in range(nodes_x):
            tile, shift = divmod(nodes_z * y, 128)
            at = node + shift
            begin = 128 * tile
            work_ref[y, pl.ds(24, 8)] = zero
            for low, high in TILES:
                here = in_ref[c, low:high, begin : begin + 128]
                got = lane_pick(here, at & 127)
                if shift + nodes_z > 128:
                    stop = min(begin + 256, width)
                    there = in_ref[c, low:high, begin + 128 : stop]
                    if stop < begin + 256:
                        there = jnp.concatenate([there, jnp.zeros((ROWS, begin + 256 - stop), F32)], 1)
                    got = jnp.where(at < 128, got, lane_pick(there, at & 127))
                work_ref[y, low:high] = jnp.where(free, got, 0.0)
        out_c = jnp.where(c == 2, 2, 1 - c)
        for i in range(N):
            for j in range(N):
                for which in range(2):
                    rows = [work_ref[DEG * ORDER[2 * which + k] + i, pl.ds(j, SIDE, stride=DEG)] for k in range(2)]
                    value = jnp.concatenate(rows, 0)
                    outs[which][out_c, i, j] = value
                    if j == 0:
                        yb_ref[out_c, i, pl.ds(2 * which, 1)] = value[:1]
                        yb_ref[out_c, i, pl.ds(2 * which + 1, 1)] = value[SIDE : SIDE + 1]
                    if i == 0 and which == 0:
                        xl_ref[out_c, j] = value[:SIDE]
        return carry

    lax.fori_loop(0, 3, component, 0)


def coeff_kernel(par_ref, coef_ref, lame_ref, material_ref, wz_ref, *outs):
    lane = lax.broadcasted_iota(jnp.int32, (ROWS, 128), 1)
    weight_z = wz_ref[...]
    for which in range(2):
        rows = [material_ref[b, ORDER[2 * which + k]][None] for k in range(2) for b in range(SIDE)]
        kind = jnp.concatenate(rows, 0).astype(F32)
        kind = jnp.concatenate([kind, jnp.zeros((ROWS, 128 - kind.shape[1]), F32)], 1)
        kind = lane_pick(kind, lane // N)
        for part in range(2):
            value = jnp.zeros((ROWS, 128), F32)
            for label in range(lame_ref.shape[1]):
                value = jnp.where(kind == float(label), lame_ref[part, label], value)
            value = value * weight_z
            for i in range(N):
                for j in range(N):
                    outs[2 * which + part][i, j] = value * float(WEIGHTS[i] * WEIGHTS[j])


def halo_corner_kernel(xr_ref, yb_ref, out_ref):
    row = lax.broadcasted_iota(jnp.int32, (SIDE, 128), 0)
    for n in range(6):
        for i in range(N):
            value = yb_ref[n, i]
            if i == DEG:
                value = jnp.where(row == 1, jnp.broadcast_to(xr_ref[n, 0][:1], (SIDE, 128)), value)
            out_ref[n, i] = value


def halo_kernel(xr_ref, yr_ref, *refs):
    fields, outs = refs[:4], refs[4:]
    row = lax.broadcasted_iota(jnp.int32, (ROWS, 128), 0)
    for n in range(2):
        for tile in range(2):
            src, dst = fields[2 * n + tile], outs[2 * n + tile]

            def plane(j, edge):
                for c in range(3):
                    for i in range(N):
                        value = src[c, i, j]
                        if tile == 0 and i == DEG:
                            face = xr_ref[3 * n + c, j]
                            value = jnp.where(row < SIDE, value, jnp.concatenate([face, face], 0))
                        if edge == 1:
                            face = yr_ref[3 * n + c, i]
                            first = jnp.broadcast_to(face[2 * tile : 2 * tile + 1], (ROWS, 128))
                            second = jnp.broadcast_to(face[2 * tile + 1 : 2 * tile + 2], (ROWS, 128))
                            value = jnp.where(row == SIDE - 1, first, jnp.where(row == ROWS - 1, second, value))
                        dst[c, i, j] = value

            over_planes(plane)


def store_kernel(t0_ref, t1_ref, out_ref, work_ref):
    nodes_x, width = out_ref.shape[1], out_ref.shape[2]
    nodes_z = width // nodes_x
    parts = (t0_ref, t1_ref)
    lane = lax.broadcasted_iota(jnp.int32, (ROWS, 128), 1)

    def component(c, carry):
        in_c = jnp.where(c == 2, 2, 1 - c)
        for i in range(DEG):
            for j in range(DEG):
                for which in range(2):
                    value = parts[which][in_c, i, j]
                    for k in range(2):
                        at = DEG * ORDER[2 * which + k] + i
                        work_ref[at, pl.ds(j, SIDE, stride=DEG)] = value[SIDE * k : SIDE * k + SIDE]
        for begin in range(0, width, 128):
            stop = min(begin + 128, width)
            for low, high in TILES:
                result = None
                for y in range(begin // nodes_z, (stop - 1) // nodes_z + 1):
                    node = jnp.clip(lane + (begin - nodes_z * y), 0, nodes_z - 1) + 1
                    got = lane_pick(work_ref[y, low:high], N * (node // DEG) + node % DEG)
                    result = got if result is None else jnp.where(lane + begin >= nodes_z * y, got, result)
                out_ref[c, low:high, begin:stop] = result[:, : stop - begin]
        return carry

    lax.fori_loop(0, 3, component, 0)


VM = pl.BlockSpec(memory_space=pltpu.VMEM)
SM = pl.BlockSpec(memory_space=pltpu.SMEM)
FIELD = (3, N, N, ROWS, 128)


def shape(dims):
    return jax.ShapeDtypeStruct(dims, F32)


def call(kernel, smem, inputs, outs, work=0, rows=FIELD):
    return pl.pallas_call(
        kernel,
        in_specs=[SM] * smem + [VM] * (len(inputs) - smem),
        out_specs=[VM] * len(outs),
        out_shape=[shape(dims) for dims in outs],
        scratch_shapes=[pltpu.VMEM(rows, F32)] * work,
        compiler_params=pltpu.CompilerParams(vmem_limit_bytes=6 << 20),
    )(*inputs)


def swaps(even, odd, axis):
    size = lax.axis_size(axis)
    got_odd = lax.ppermute(odd, axis, [(i, (((i + 1) ^ 1) - 1) % size) for i in range(size)])
    got_even = lax.ppermute(even, axis, [(i, i ^ 1) for i in range(size)])
    return got_even, got_odd


def exchange(par, x_faces, fields):
    xe, xo = swaps(*x_faces, "gy")
    ye, yo = call(corner_kernel, 1, (par, xe, xo, *fields), (xe.shape, xe.shape))
    ye, yo = swaps(ye, yo, "gx")
    return xe, xo, ye, yo


def from_next(value, axis):
    size = lax.axis_size(axis)
    return lax.ppermute(value, axis, [(i, (i - 1) % size) for i in range(size)])


def local(right_side, guess, material, lame, upper, lower_ratio):
    elems_x, elems_y, elems_z = material.shape
    nodes_y = DEG * elems_y
    w_grad, w_back, w_share = z_matrices(elems_z)
    w_grad = jnp.asarray(w_grad, BF16)
    w_back = jnp.asarray(w_back, BF16)
    w_share = jnp.asarray(w_share, BF16)
    par = jnp.stack([lax.axis_index("gy") % 2, lax.axis_index("gx") % 2]).astype(jnp.int32)

    upper_edge = upper[0]
    lower_edge = lower_ratio[0] * upper_edge
    center = (upper_edge + lower_edge) / 2.0
    radius = (upper_edge - lower_edge) / 2.0
    sigma_ratio = center / radius
    pairs = [(jnp.zeros((), F32), 1.0 / center)]
    factor = 1.0 / sigma_ratio
    for step_index in range(CHEB - 1):
        factor_next = 1.0 / (2.0 * sigma_ratio - factor)
        pairs.append((factor_next * factor, 2.0 * factor_next / radius))
        factor = factor_next
    coef = jnp.stack([value for pair in pairs for value in pair]).astype(F32)
    grid = (N, N, ROWS, 128)
    weight_z = jnp.asarray(np.tile(WEIGHTS, (ROWS, elems_z)), F32)
    coeffs = call(coeff_kernel, 3, (par, coef, lame, material, weight_z), (grid,) * 4)
    coeffs = [coeffs[:2], coeffs[2:]]

    plane = (3, N, SIDE, 128)
    staged = (nodes_y + 1, nodes_y + SIDE, 128)
    loads = [call(load_kernel, 2, (par, coef, value), (FIELD, FIELD, plane, plane), 1, staged) for value in (guess, right_side)]
    x_halo = from_next(jnp.concatenate([load[2] for load in loads], 0), "gy")
    y_halo = jnp.concatenate([load[3] for load in loads], 0)
    (y_halo,) = call(halo_corner_kernel, 0, (x_halo, y_halo), (y_halo.shape,))
    y_halo = from_next(y_halo, "gx")
    u0, u1, b0, b1 = call(halo_kernel, 0, (x_halo, y_halo, *loads[0][:2], *loads[1][:2]), (FIELD,) * 4)
    u, b = [u0, u1], [b0, b1]

    ratio_z = jnp.asarray(np.tile(RATIO, (ROWS, elems_z)), F32)

    weights = (w_grad, w_back, w_share)
    au = [None, None]
    diag = [None, None]
    for tile in range(2):
        lam_w, mu_w = coeffs[tile][0], coeffs[tile][1]
        faces = ((6, N, SIDE, 128),) * (0 if tile else 2)
        au[tile], diag[tile], *got_faces = call(
            lambda *refs, tile=tile: first_kernel(tile, *refs), 2,
            (par, jnp.asarray(RATIO, F32), u[tile], lam_w, mu_w, ratio_z, *weights), (FIELD, FIELD) + faces, 3,
        )
        x_faces = x_faces if tile else got_faces
    fields = (*au, *diag)
    change = [None, None]
    inv = [None, None]
    for count in range(SWEEPS * CHEB):
        got = exchange(par, x_faces, fields)
        stage = count % CHEB
        with_diag = count == 0
        old_au, au = au, [None, None]
        for tile in range(2):
            lam_w, mu_w = coeffs[tile][0], coeffs[tile][1]
            inputs = (par, coef, u[tile], b[tile], *old_au, *got)
            inputs += tuple(diag) if with_diag else (inv[tile],)
            inputs += () if stage == 0 else (change[tile],)
            inputs += (lam_w, mu_w, *weights)
            outs = (FIELD, FIELD, FIELD) + ((FIELD,) if with_diag else ())
            outs += () if tile else ((3, N, SIDE, 128),) * 2

            def kernel(*refs, flags=(tile, stage, with_diag)):
                step_kernel(*flags, *refs)

            results = list(call(kernel, 2, inputs, outs, 3))
            u[tile], change[tile], au[tile] = results[:3]
            if with_diag:
                inv[tile] = results[3]
            if tile == 0:
                x_faces = results[-2:]
        fields = au
    got = exchange(par, x_faces, fields)
    residual = call(last_kernel, 1, (par, *b, *au, *got), (FIELD, FIELD))

    def to_nodes(field):
        return call(store_kernel, 0, tuple(field), (guess.shape,), 1, staged)[0]

    return (to_nodes(u), to_nodes(residual))


def solution(mesh):
    placed = (P(None, "gx", "gy"), P(None, "gx", "gy"), P("gx", "gy", None), P(), P(), P())
    return jax.shard_map(
        local,
        mesh=mesh,
        in_specs=placed,
        out_specs=(P(None, "gx", "gy"), P(None, "gx", "gy")),
        check_vma=False,
    )
```

```python
import jax
import jax.numpy as jnp
import numpy as np
from jax import lax
from jax.experimental import pallas as pl
from jax.experimental.pallas import tpu as pltpu
from jax.sharding import PartitionSpec as P

DEG = 7
N = DEG + 1
SWEEPS = 2
CHEB = 3
F32 = jnp.float32
BF16 = jnp.bfloat16
highest = lax.Precision.HIGHEST


def legendre_pair(points, degree):
    prev_poly = points * 0.0 + 1.0
    this_poly = points * 1.0
    for order in range(2, degree + 1):
        next_poly = ((2 * order - 1) * points * this_poly - (order - 1) * prev_poly) / order
        prev_poly = this_poly
        this_poly = next_poly
    return (this_poly, prev_poly)


def gll_tables(degree):
    count = degree + 1
    points = -np.cos(np.pi * np.arange(count) / degree)
    for newton_step in range(60):
        this_poly, prev_poly = legendre_pair(points, degree)
        points = points - (points * this_poly - prev_poly) / (count * this_poly)
    values, unused_poly = legendre_pair(points, degree)
    weights = 2.0 / (degree * (degree + 1) * values**2)
    identity_np = np.eye(count)
    spacing = points[:, None] - points[None, :] + identity_np
    derivative = values[:, None] / (values[None, :] * spacing) * (1.0 - identity_np)
    derivative[0, 0] = -degree * (degree + 1) / 4.0
    derivative[degree, degree] = degree * (degree + 1) / 4.0
    stiff_ratio = (weights[:, None] * derivative**2).sum(0) / weights
    return (weights, derivative, stiff_ratio)


WEIGHTS, DERIV, RATIO = gll_tables(DEG)


def halves(matrix):
    high = matrix.astype(BF16).astype(np.float32)
    low = matrix.astype(np.float32) - high
    return high, low


def z_matrices(blocks):
    width = blocks * N
    node = np.array([DEG * f + k for f in range(blocks) for k in range(N)])
    free = (node > 0) & (node < DEG * blocks)
    share = ((node[:, None] == node[None, :]) & free[:, None] & free[None, :]).astype(np.float64)
    grad = np.kron(np.eye(blocks), DERIV.T)
    back = np.kron(np.eye(blocks), DERIV) @ share
    zero = np.zeros((width, width))
    grad_hi, grad_lo = halves(grad)
    back_hi, back_lo = halves(back)
    w_grad = np.block([[grad_hi, grad_lo], [grad_hi, zero]])
    w_back = np.block([[back_hi, back_lo], [back_hi, zero]])
    w_share = np.concatenate([share, share], 0)
    return w_grad, w_back, w_share


def line_sums(vals, matrix, pairs=range(N // 2)):
    even = [vals[i] + vals[DEG - i] for i in range(N // 2)]
    odd = [vals[i] - vals[DEG - i] for i in range(N // 2)]
    outs = [None] * N
    for p in pairs:
        from_even = None
        from_odd = None
        for i in range(N // 2):
            te = float(np.float32((matrix[p, i] + matrix[p, DEG - i]) / 2.0)) * even[i]
            to = float(np.float32((matrix[p, i] - matrix[p, DEG - i]) / 2.0)) * odd[i]
            from_even = te if from_even is None else from_even + te
            from_odd = to if from_odd is None else from_odd + to
        outs[p] = from_odd + from_even
        outs[DEG - p] = from_odd - from_even
    return outs


def split_pair(value):
    high = value.astype(BF16)
    low = (value - high.astype(F32)).astype(BF16)
    return jnp.concatenate([high, low], axis=-1)


def dot(a, b):
    return jnp.dot(a, b, preferred_element_type=F32)


ROWS = 8
SIDE = 4
ORDER = (0, 3, 1, 2)
UNROLL = 2


def flip(value):
    return jnp.concatenate([value[SIDE:], value[:SIDE]], 0)


def whole(ref):
    return lambda c, i, j: ref[c, i, j]


def by_i(face_ref, inner_ref):
    return lambda c, i, j: face_ref[c, i // DEG, j] if i in (0, DEG) else inner_ref[c, i - 1, j]


def by_j(mid_ref, edge_ref):
    return lambda c, i, j: edge_ref[c, i, j // DEG] if j in (0, DEG) else mid_ref[c, i, j - 1]


def received(ctl_ref, axis, even_ref, odd_ref, *at):
    is_even = ctl_ref[axis][:SIDE] < 0.5
    even = even_ref[at]
    odd = odd_ref[at]
    return jnp.where(is_even, even, odd), jnp.where(is_even, odd, even)


def sum_x(ctl_ref, xe_ref, xo_ref, parts, c, face_at, i, j, tile):
    total = parts[tile](c, i, j)
    if 0 < i < DEG:
        return total
    row = lax.broadcasted_iota(jnp.int32, (ROWS, 128), 0)
    across = DEG - i
    if tile == 0:
        right, left = received(ctl_ref, 0, xe_ref, xo_ref, face_at, j)
        face = right if i else left
        face = jnp.concatenate([face, face], 0)
        inner = parts[1](c, across, j)
        low, high = (inner, face) if i else (face, inner)
    else:
        middle = flip(parts[1](c, across, j))
        outer = parts[0](c, across, j)
        low, high = (middle, outer) if i else (outer, middle)
    return total + jnp.where(row < SIDE, low, high)


def sum_all(ctl_ref, faces, parts, c, face_at, i, j, tile):
    xe, xo, ye, yo = faces
    total = sum_x(ctl_ref, xe, xo, parts, c, face_at, i, j, tile)
    if j in (0, DEG):
        row = lax.broadcasted_iota(jnp.int32, (ROWS, 128), 0)
        top, bottom = received(ctl_ref, 1, ye, yo, face_at, i)
        face = top if j else bottom
        at = SIDE - 1 if j else 0
        first = jnp.broadcast_to(face[2 * tile : 2 * tile + 1], (ROWS, 128))
        second = jnp.broadcast_to(face[2 * tile + 1 : 2 * tile + 2], (ROWS, 128))
        total = total + jnp.where(row == at, first, jnp.where(row == SIDE + at, second, 0.0))
    return total


def loop(count, body, unroll=UNROLL):
    def inner(i, carry):
        body(i)
        return carry

    lax.fori_loop(0, count, inner, 0, unroll=unroll)


def gradients(planes, at, wg_ref, gx_ref, gz_ref):
    flat = jnp.concatenate([planes[c][i] for c in range(3) for i in range(N)], 0)
    both = dot(split_pair(flat), wg_ref[...])
    for c in range(3):
        outs = line_sums(planes[c], DERIV)
        for i in range(N):
            gx_ref[c, i, at] = outs[i]
    both = (both[:, :128] + both[:, 128:]).reshape(3, N, ROWS, 128)
    for c in range(3):
        for i in range(N):
            gz_ref[c, i, at] = both[c, i]


def stress(u_at, gx_at, gz_at, lam_ref, mu_ref, wb_ref, sx_ref, fz_ref, fy_ref):
    def plane(i):
        gy = [line_sums([u_at(c, i, j) for j in range(N)], DERIV) for c in range(3)]
        sy = [[None] * N for c in range(3)]
        sz = [[None] * N for c in range(3)]
        for j in range(N):
            gx = [gx_at(c, i, j) for c in range(3)]
            gz = [gz_at(c, i, j) for c in range(3)]
            mu = mu_ref[i, j]
            mu2 = mu + mu
            trace = lam_ref[i, j] * (gx[0] + gy[1][j] + gz[2])
            sxy = mu * (gx[1] + gy[0][j])
            sxz = mu * (gx[2] + gz[0])
            syz = mu * (gy[2][j] + gz[1])
            sx_ref[0, i, j] = mu2 * gx[0] + trace
            sx_ref[1, i, j] = sxy
            sx_ref[2, i, j] = sxz
            sz[0][j] = sxz
            sz[1][j] = syz
            sz[2][j] = mu2 * gz[2] + trace
            sy[0][j] = sxy
            sy[1][j] = mu2 * gy[1][j] + trace
            sy[2][j] = syz
        flat = jnp.concatenate([sz[c][j] for c in range(3) for j in range(N)], 0)
        both = dot(split_pair(flat), wb_ref[...])
        for c in range(3):
            outs = line_sums(sy[c], DERIV.T)
            for j in range(N):
                fy_ref[c, i, j] = outs[j]
        both = (both[:, :128] + both[:, 128:]).reshape(3, N, ROWS, 128)
        for c in range(3):
            fz_ref[c, i] = both[c]

    loop(N, plane)


def back(ws_ref, work, out_ref, nodes, planes):
    sx_ref, fz_ref, fy_ref = work
    pairs = sorted({min(i, DEG - i) for i in nodes})
    flat = []
    for j in planes:
        for c in range(3):
            outs = line_sums([sx_ref[c, i, j] for i in range(N)], DERIV.T, pairs)
            flat += [outs[i] + fy_ref[c, i, j] for i in nodes]
    both = dot(split_pair(jnp.concatenate(flat, 0)), ws_ref[...]).reshape(len(planes), 3, len(nodes), ROWS, 128)
    for at, j in enumerate(planes):
        for c in range(3):
            for k, i in enumerate(nodes):
                out_ref[c, k, j] = both[at, c, k] + fz_ref[c, i, j]


def back_loop(ws_ref, work, out_ref, nodes):
    loop(N, lambda j: back(ws_ref, work, out_ref, nodes, (j,)))


def join_y(part_ref):
    row = lax.broadcasted_iota(jnp.int32, (ROWS, 128), 0)
    near = row % SIDE

    def along(i):
        for c in range(3):
            last = part_ref[c, i, DEG]
            start = part_ref[c, i, 0]
            last = last + jnp.where(near < SIDE - 1, jnp.concatenate([start[1:], start[:1]], 0), 0.0)
            start = jnp.where(near > 0, jnp.concatenate([last[-1:], last[:-1]], 0), start)
            part_ref[c, i, DEG] = last
            part_ref[c, i, 0] = start

    loop(part_ref.shape[1], along)


def give_faces(ctl_ref, part_ref, first, xe_ref, xo_ref):
    is_even = ctl_ref[0][:SIDE] < 0.5
    end = part_ref.shape[1] - 1

    def plane(j):
        for c in range(3):
            right = part_ref[c, end, j][SIDE:]
            left = part_ref[c, 0, j][:SIDE]
            xe_ref[first + c, j] = jnp.where(is_even, right, left)
            xo_ref[first + c, j] = jnp.where(is_even, left, right)

    loop(N, plane)


ENDS = (0, DEG)
INSIDE = tuple(range(1, DEG))
ALL = tuple(range(N))


def send_first(ctl_ref, ws_ref, work, face_ref, xe_ref, xo_ref):
    back(ws_ref, work, face_ref, ENDS, ALL)
    join_y(face_ref)
    give_faces(ctl_ref, face_ref, 0, xe_ref, xo_ref)


def finish_second(ws_ref, work, work_0, inner_ref, au_ref):
    back_loop(ws_ref, work, au_ref, ALL)
    join_y(au_ref)
    back_loop(ws_ref, work_0, inner_ref, INSIDE)
    join_y(inner_ref)


def first_kernel(tile, *refs):
    refs = list(refs)
    take = lambda count: [refs.pop(0) for _ in range(count)]
    ctl_ref, mid_ref, edge_ref, lam_ref, mu_ref, ratio_ref, rk_ref, wg_ref, wb_ref, ws_ref = take(10)
    if tile == 0:
        dg_ref, face_ref, xe_ref, xo_ref = take(4)
    else:
        work_0 = take(3)
        dg_ref, inner_ref, au_ref = take(3)
    sx_ref, fz_ref, fy_ref = take(3)

    def diagonal(i):
        rows = [[None] * N for c in range(3)]
        for j in range(N):
            lam = lam_ref[i, j]
            mu = mu_ref[i, j]
            ri = ratio_ref[i]
            rk = rk_ref[...]
            total = rk + (ri + float(RATIO[j]))
            for c in range(3):
                own = (ri, float(RATIO[j]), rk)[c]
                rows[c][j] = lam * own + mu * (total + own)
        flat = jnp.concatenate([rows[c][j] for c in range(3) for j in range(N)], 0)
        both = dot(split_pair(flat), ws_ref[...]).reshape(3, N, ROWS, 128)
        for c in range(3):
            dg_ref[c, i] = both[c]

    loop(N, diagonal, 1)

    def start(at):
        gradients([[mid_ref[c, i, at] for i in range(N)] for c in range(3)], at + 1, wg_ref, sx_ref, fz_ref)

    loop(N - 2, start)
    for k in range(2):
        gradients([[edge_ref[c, i, k] for i in range(N)] for c in range(3)], DEG * k, wg_ref, sx_ref, fz_ref)
    work = (sx_ref, fz_ref, fy_ref)
    stress(by_j(mid_ref, edge_ref), whole(sx_ref), whole(fz_ref), lam_ref, mu_ref, wb_ref, *work)
    join_y(dg_ref)
    if tile == 0:
        send_first(ctl_ref, ws_ref, work, face_ref, xe_ref, xo_ref)
        give_faces(ctl_ref, dg_ref, 3, xe_ref, xo_ref)
    else:
        finish_second(ws_ref, work, work_0, inner_ref, au_ref)


def corner_kernel(ctl_ref, xe_ref, xo_ref, face_ref, inner_ref, au_ref, *refs):
    ye_ref, yo_ref = refs[-2:]
    fields = [(by_i(face_ref, inner_ref), whole(au_ref))]
    if len(refs) > 2:
        fields.append((whole(refs[0]), whole(refs[1])))
    is_even = ctl_ref[1][:SIDE] < 0.5
    for n, parts in enumerate(fields):
        for c in range(3):
            at = 3 * n + c
            for i in range(N):
                rows_t = []
                rows_b = []
                for tile in range(2):
                    top = sum_x(ctl_ref, xe_ref, xo_ref, parts, c, at, i, DEG, tile)
                    bottom = sum_x(ctl_ref, xe_ref, xo_ref, parts, c, at, i, 0, tile)
                    rows_t += [top[SIDE - 1 : SIDE], top[-1:]]
                    rows_b += [bottom[:1], bottom[SIDE : SIDE + 1]]
                top = jnp.concatenate(rows_t, 0)
                bottom = jnp.concatenate(rows_b, 0)
                ye_ref[at, i] = jnp.where(is_even, top, bottom)
                yo_ref[at, i] = jnp.where(is_even, bottom, top)


def invert(diag):
    lane = lax.broadcasted_iota(jnp.int32, (ROWS, 128), 1)
    clamped = (lane == 0) | (lane == 127)
    return jnp.where(clamped, 0.0, 1.0 / jnp.where(clamped, 1.0, diag))


def advance(ctl_ref, stage, u, load, total, inv, change):
    change_new = ctl_ref[3 + 2 * stage] * (inv * (load - total))
    if stage:
        change_new = ctl_ref[2 + 2 * stage] * change + change_new
    return u + change_new, change_new


def mid_kernel(stage, with_diag, *refs):
    refs = list(refs)
    take = lambda count: [refs.pop(0) for _ in range(count)]
    ctl_ref, wg_ref, face_ref, inner_ref, au_ref, xe_ref, xo_ref = take(7)
    parts = (by_i(face_ref, inner_ref), whole(au_ref))
    diag_parts = [whole(ref) for ref in take(2)] if with_diag else None
    ins = []
    for tile in range(2):
        u_ref, b_ref = take(2)
        ins.append((u_ref, b_ref, None if with_diag else take(1)[0], take(1)[0] if stage else None))
    for tile in range(2):
        u_ref, b_ref, inv_ref, change_ref = ins[tile]
        u_out, change_out, gx_ref, gz_ref = take(4)
        inv_out = take(1)[0] if with_diag else None

        def plane(at):
            j = at + 1
            planes = [[None] * N for c in range(3)]
            for c in range(3):
                for i in range(N):
                    if with_diag:
                        inv = invert(sum_x(ctl_ref, xe_ref, xo_ref, diag_parts, c, 3 + c, i, j, tile))
                        inv_out[c, i, at] = inv
                    else:
                        inv = inv_ref[c, i, at]
                    total = sum_x(ctl_ref, xe_ref, xo_ref, parts, c, c, i, j, tile)
                    change = change_ref[c, i, at] if stage else None
                    planes[c][i], change = advance(ctl_ref, stage, u_ref[c, i, at], b_ref[c, i, j], total, inv, change)
                    change_out[c, i, at] = change
                    u_out[c, i, at] = planes[c][i]
            gradients(planes, at, wg_ref, gx_ref, gz_ref)

        loop(N - 2, plane)


def edge_kernel(tile, stage, with_diag, *refs):
    refs = list(refs)
    take = lambda count: [refs.pop(0) for _ in range(count)]
    ctl_ref, wg_ref, wb_ref, ws_ref, lam_ref, mu_ref, face_in, inner_in, au_in = take(9)
    faces = take(4)
    parts = (by_i(face_in, inner_in), whole(au_in))
    diag_parts = [whole(ref) for ref in take(2)] if with_diag else None
    mid_ref, gx_ref, gz_ref, u_ref, b_ref = take(5)
    inv_ref = None if with_diag else take(1)[0]
    change_ref = take(1)[0] if stage else None
    work_0 = take(3) if tile else None
    u_out, change_out = take(2)
    inv_out = take(1)[0] if with_diag else None
    outs = take(2 if tile else 3)
    work = take(3)
    sx_ref, fz_ref, fy_ref = work
    for k in range(2):
        j = DEG * k
        planes = [[None] * N for c in range(3)]
        for c in range(3):
            for i in range(N):
                if with_diag:
                    inv = invert(sum_all(ctl_ref, faces, diag_parts, c, 3 + c, i, j, tile))
                    inv_out[c, i, k] = inv
                else:
                    inv = inv_ref[c, i, k]
                total = sum_all(ctl_ref, faces, parts, c, c, i, j, tile)
                change = change_ref[c, i, k] if stage else None
                planes[c][i], change = advance(ctl_ref, stage, u_ref[c, i, k], b_ref[c, i, j], total, inv, change)
                change_out[c, i, k] = change
                u_out[c, i, k] = planes[c][i]
        gradients(planes, j, wg_ref, sx_ref, fz_ref)

    def mixed(mid, full):
        return lambda c, i, j: full[c, i, j] if j in ENDS else mid[c, i, j - 1]

    stress(by_j(mid_ref, u_out), mixed(gx_ref, sx_ref), mixed(gz_ref, fz_ref), lam_ref, mu_ref, wb_ref, *work)
    if tile == 0:
        send_first(ctl_ref, ws_ref, work, *outs)
    else:
        finish_second(ws_ref, work, work_0, *outs)


def lane_pick(value, index):
    return jnp.take_along_axis(value, index, axis=1, mode="promise_in_bounds")


TILES = ((0, 8), (8, 16), (16, 24), (20, 28))


def load_kernel(ctl_ref, in_ref, t0_ref, t1_ref, xl_ref, yb_ref, work_ref):
    nodes_x, width = in_ref.shape[1], in_ref.shape[2]
    nodes_z = width // nodes_x
    outs = (t0_ref, t1_ref)
    lane = lax.broadcasted_iota(jnp.int32, (ROWS, 128), 1)
    node = DEG * (lane // N) + lane % N - 1
    free = (node >= 0) & (node < nodes_z)
    node = jnp.clip(node, 0, nodes_z - 1)
    zero = jnp.zeros((ROWS, 128), F32)
    for r in range(4):
        work_ref[nodes_x, pl.ds(8 * r, 8)] = zero

    def component(c, carry):
        for y in range(nodes_x):
            tile, shift = divmod(nodes_z * y, 128)
            at = node + shift
            begin = 128 * tile
            work_ref[y, pl.ds(24, 8)] = zero
            for low, high in TILES:
                here = in_ref[c, low:high, begin : begin + 128]
                got = lane_pick(here, at & 127)
                if shift + nodes_z > 128:
                    stop = min(begin + 256, width)
                    there = in_ref[c, low:high, begin + 128 : stop]
                    if stop < begin + 256:
                        there = jnp.concatenate([there, jnp.zeros((ROWS, begin + 256 - stop), F32)], 1)
                    got = jnp.where(at < 128, got, lane_pick(there, at & 127))
                work_ref[y, low:high] = jnp.where(free, got, 0.0)
        out_c = jnp.where(c == 2, 2, 1 - c)
        for i in range(N):
            for j in range(N):
                for which in range(2):
                    rows = [work_ref[DEG * ORDER[2 * which + k] + i, pl.ds(j, SIDE, stride=DEG)] for k in range(2)]
                    value = jnp.concatenate(rows, 0)
                    outs[which][out_c, i, j] = value
                    if j == 0:
                        yb_ref[out_c, i, pl.ds(2 * which, 1)] = value[:1]
                        yb_ref[out_c, i, pl.ds(2 * which + 1, 1)] = value[SIDE : SIDE + 1]
                    if i == 0 and which == 0:
                        xl_ref[out_c, j] = value[:SIDE]
        return carry

    lax.fori_loop(0, 3, component, 0)


def coeff_kernel(lame_ref, ctl_ref, material_ref, wz_ref, *outs):
    lane = lax.broadcasted_iota(jnp.int32, (ROWS, 128), 1)
    weight_z = wz_ref[...]
    for which in range(2):
        rows = [material_ref[b, ORDER[2 * which + k]][None] for k in range(2) for b in range(SIDE)]
        kind = jnp.concatenate(rows, 0).astype(F32)
        kind = jnp.concatenate([kind, jnp.zeros((ROWS, 128 - kind.shape[1]), F32)], 1)
        kind = lane_pick(kind, lane // N)
        for part in range(2):
            value = jnp.zeros((ROWS, 128), F32)
            for label in range(lame_ref.shape[1]):
                value = jnp.where(kind == float(label), lame_ref[part, label], value)
            value = value * weight_z
            for i in range(N):
                for j in range(N):
                    outs[2 * which + part][i, j] = value * float(WEIGHTS[i] * WEIGHTS[j])


def halo_corner_kernel(xr_ref, yb_ref, out_ref):
    row = lax.broadcasted_iota(jnp.int32, (SIDE, 128), 0)
    for n in range(6):
        for i in range(N):
            value = yb_ref[n, i]
            if i == DEG:
                value = jnp.where(row == 1, jnp.broadcast_to(xr_ref[n, 0][:1], (SIDE, 128)), value)
            out_ref[n, i] = value


def halo_kernel(xr_ref, yr_ref, *refs):
    fields, outs = refs[:4], refs[4:]
    row = lax.broadcasted_iota(jnp.int32, (ROWS, 128), 0)
    for n in range(2):
        for tile in range(2):
            src = fields[2 * n + tile]
            mid_ref, edge_ref = outs[2 * tile : 2 * tile + 2]
            dst = outs[4 + tile]

            def plane(j):
                for c in range(3):
                    for i in range(N):
                        value = src[c, i, j]
                        if tile == 0 and i == DEG:
                            face = xr_ref[3 * n + c, j]
                            value = jnp.where(row < SIDE, value, jnp.concatenate([face, face], 0))
                        if j is DEG:
                            face = yr_ref[3 * n + c, i]
                            first = jnp.broadcast_to(face[2 * tile : 2 * tile + 1], (ROWS, 128))
                            second = jnp.broadcast_to(face[2 * tile + 1 : 2 * tile + 2], (ROWS, 128))
                            value = jnp.where(row == SIDE - 1, first, jnp.where(row == ROWS - 1, second, value))
                        if n == 1:
                            dst[c, i, j] = value
                        elif isinstance(j, int):
                            edge_ref[c, i, j // DEG] = value
                        else:
                            mid_ref[c, i, j - 1] = value

            plane(0)
            loop(N - 2, lambda at: plane(at + 1), 1)
            plane(DEG)


def store_kernel(with_residual, *refs):
    refs = list(refs)
    take = lambda count: [refs.pop(0) for _ in range(count)]
    if with_residual:
        ctl_ref, b0_ref, b1_ref, face_ref, inner_ref, au_ref = take(6)
        faces = take(4)
        sums = (by_i(face_ref, inner_ref), whole(au_ref))
        loads = (whole(b0_ref), whole(b1_ref))
        parts = [
            lambda c, i, j, tile=tile: loads[tile](c, i, j) - sum_all(ctl_ref, faces, sums, c, c, i, j, tile)
            for tile in range(2)
        ]
    else:
        parts = [by_j(*take(2)) for tile in range(2)]
    out_ref, work_ref = refs
    nodes_x, width = out_ref.shape[1], out_ref.shape[2]
    nodes_z = width // nodes_x
    lane = lax.broadcasted_iota(jnp.int32, (ROWS, 128), 1)

    def component(c, carry):
        in_c = jnp.where(c == 2, 2, 1 - c)
        for i in range(DEG):
            for j in range(DEG):
                for which in range(2):
                    value = parts[which](in_c, i, j)
                    for k in range(2):
                        at = DEG * ORDER[2 * which + k] + i
                        work_ref[at, pl.ds(j, SIDE, stride=DEG)] = value[SIDE * k : SIDE * k + SIDE]
        for begin in range(0, width, 128):
            stop = min(begin + 128, width)
            for low, high in TILES:
                result = None
                for y in range(begin // nodes_z, (stop - 1) // nodes_z + 1):
                    node = jnp.clip(lane + (begin - nodes_z * y), 0, nodes_z - 1) + 1
                    got = lane_pick(work_ref[y, low:high], N * (node // DEG) + node % DEG)
                    result = got if result is None else jnp.where(lane + begin >= nodes_z * y, got, result)
                out_ref[c, low:high, begin:stop] = result[:, : stop - begin]
        return carry

    lax.fori_loop(0, 3, component, 0)


VM = pl.BlockSpec(memory_space=pltpu.VMEM)
SM = pl.BlockSpec(memory_space=pltpu.SMEM)
FIELD = (3, N, N, ROWS, 128)
MID = (3, N, N - 2, ROWS, 128)
EDGE = (3, N, 2, ROWS, 128)
FACE = (3, 2, N, ROWS, 128)
INNER = (3, N - 2, N, ROWS, 128)


def shape(dims):
    return jax.ShapeDtypeStruct(dims, F32)


def call(kernel, smem, inputs, outs, work=0, rows=FIELD):
    return pl.pallas_call(
        kernel,
        in_specs=[SM] * smem + [VM] * (len(inputs) - smem),
        out_specs=[VM] * len(outs),
        out_shape=[shape(dims) for dims in outs],
        scratch_shapes=[pltpu.VMEM(rows, F32)] * work,
        compiler_params=pltpu.CompilerParams(vmem_limit_bytes=6 << 20),
    )(*inputs)


def swaps(even, odd, axis):
    size = lax.axis_size(axis)
    got_odd = lax.ppermute(odd, axis, [(i, (((i + 1) ^ 1) - 1) % size) for i in range(size)])
    got_even = lax.ppermute(even, axis, [(i, i ^ 1) for i in range(size)])
    return got_even, got_odd


def exchange(ctl, x_faces, fields):
    xe, xo = swaps(*x_faces, "gy")
    ye, yo = call(corner_kernel, 0, (ctl, xe, xo, *fields), (xe.shape, xe.shape))
    ye, yo = swaps(ye, yo, "gx")
    return (xe, xo), (ye, yo)


def from_next(value, axis):
    size = lax.axis_size(axis)
    return lax.ppermute(value, axis, [(i, (i - 1) % size) for i in range(size)])


def local(right_side, guess, material, lame, upper, lower_ratio):
    elems_x, elems_y, elems_z = material.shape
    nodes_y = DEG * elems_y
    w_grad, w_back, w_share = z_matrices(elems_z)
    w_grad = jnp.asarray(w_grad, BF16)
    w_back = jnp.asarray(w_back, BF16)
    w_share = jnp.asarray(w_share, BF16)
    upper_edge = upper[0]
    lower_edge = lower_ratio[0] * upper_edge
    center = (upper_edge + lower_edge) / 2.0
    radius = (upper_edge - lower_edge) / 2.0
    sigma_ratio = center / radius
    pairs = [(jnp.zeros((), F32), 1.0 / center)]
    factor = 1.0 / sigma_ratio
    for step_index in range(CHEB - 1):
        factor_next = 1.0 / (2.0 * sigma_ratio - factor)
        pairs.append((factor_next * factor, 2.0 * factor_next / radius))
        factor = factor_next
    flags = [(lax.axis_index(axis) % 2).astype(F32) for axis in ("gy", "gx")]
    ctl = jnp.stack(flags + [value for pair in pairs for value in pair])
    ctl = jnp.broadcast_to(ctl[:, None, None], (2 + 2 * CHEB, ROWS, 128))
    grid = (N, N, ROWS, 128)
    weight_z = jnp.asarray(np.tile(WEIGHTS, (ROWS, elems_z)), F32)
    coeffs = call(coeff_kernel, 1, (lame, ctl, material, weight_z), (grid,) * 4)
    coeffs = [coeffs[:2], coeffs[2:]]

    plane = (3, N, SIDE, 128)
    staged = (nodes_y + 1, nodes_y + SIDE, 128)
    loads = [call(load_kernel, 0, (ctl, value), (FIELD, FIELD, plane, plane), 1, staged) for value in (guess, right_side)]
    x_halo = from_next(jnp.concatenate([load[2] for load in loads], 0), "gy")
    y_halo = jnp.concatenate([load[3] for load in loads], 0)
    (y_halo,) = call(halo_corner_kernel, 0, (x_halo, y_halo), (y_halo.shape,))
    y_halo = from_next(y_halo, "gx")
    *nodes, b0, b1 = call(
        halo_kernel, 0, (x_halo, y_halo, *loads[0][:2], *loads[1][:2]), (MID, EDGE, MID, EDGE, FIELD, FIELD)
    )
    u_mid = [nodes[0], nodes[2]]
    u_edge = [nodes[1], nodes[3]]
    b = [b0, b1]

    ratio_z = jnp.asarray(np.tile(RATIO, (ROWS, elems_z)), F32)
    ratio_i = jnp.asarray(np.broadcast_to(RATIO[:, None, None], (N, ROWS, 128)), F32)
    weights = (w_grad, w_back, w_share)
    work = (FIELD,) * 3
    both_faces = ((6, N, SIDE, 128),) * 2

    def first(tile, extra, outs, scratch):
        inputs = (ctl, u_mid[tile], u_edge[tile], *coeffs[tile], ratio_i, ratio_z, *weights, *extra)
        return call(lambda *refs: first_kernel(tile, *refs), 0, inputs, (FIELD,) + outs, scratch)

    diag_0, face, *rest = first(0, (), (FACE, *both_faces, *work), 0)
    x_faces, work_0 = rest[:2], rest[2:]
    diag_1, inner, au = first(1, work_0, (INNER, FIELD), 3)
    diag = (diag_0, diag_1)
    change_mid = [None, None]
    change_edge = [None, None]
    inv_mid = [None, None]
    inv_edge = [None, None]
    for count in range(SWEEPS * CHEB):
        stage = count % CHEB
        with_diag = count == 0
        sums = (face, inner, au)
        x_got, y_got = exchange(ctl, x_faces, sums + (diag if with_diag else ()))
        keep_inv = 1 if with_diag else 0

        inputs = (ctl, w_grad, *sums, *x_got) + (diag if with_diag else ())
        for tile in range(2):
            inputs += (u_mid[tile], b[tile]) + (() if with_diag else (inv_mid[tile],))
            inputs += (change_mid[tile],) if stage else ()
        outs = (MID,) * (4 + keep_inv) * 2
        results = call(lambda *refs: mid_kernel(stage, with_diag, *refs), 0, inputs, outs)
        slopes = [None, None]
        for tile in range(2):
            got = results[(4 + keep_inv) * tile : (4 + keep_inv) * (tile + 1)]
            u_mid[tile], change_mid[tile] = got[:2]
            slopes[tile] = got[2:4]
            if with_diag:
                inv_mid[tile] = got[4]

        for tile in range(2):
            inputs = (ctl, *weights, *coeffs[tile], *sums, *x_got, *y_got) + (diag if with_diag else ())
            inputs += (u_mid[tile], *slopes[tile], u_edge[tile], b[tile])
            inputs += () if with_diag else (inv_edge[tile],)
            inputs += (change_edge[tile],) if stage else ()
            inputs += tuple(work_0) if tile else ()
            outs = (EDGE,) * (2 + keep_inv)
            outs += (INNER, FIELD) if tile else (FACE, *((3, N, SIDE, 128),) * 2, *work)
            results = list(
                call(lambda *refs: edge_kernel(tile, stage, with_diag, *refs), 0, inputs, outs, 3 if tile else 0)
            )
            u_edge[tile], change_edge[tile] = results[:2]
            if with_diag:
                inv_edge[tile] = results[2]
            results = results[2 + keep_inv :]
            if tile:
                inner, au = results
            else:
                face, x_faces, work_0 = results[0], results[1:3], results[3:]
    sums = (face, inner, au)
    x_got, y_got = exchange(ctl, x_faces, sums)

    def store(with_residual, inputs):
        return call(lambda *refs: store_kernel(with_residual, *refs), 0, inputs, (guess.shape,), 1, staged)[0]

    smoothed = store(False, (u_mid[0], u_edge[0], u_mid[1], u_edge[1]))
    return (smoothed, store(True, (ctl, *b, *sums, *x_got, *y_got)))


def solution(mesh):
    placed = (P(None, "gx", "gy"), P(None, "gx", "gy"), P("gx", "gy", None), P(), P(), P())
    return jax.shard_map(
        local,
        mesh=mesh,
        in_specs=placed,
        out_specs=(P(None, "gx", "gy"), P(None, "gx", "gy")),
        check_vma=False,
    )
```

```python
import jax
import jax.numpy as jnp
import numpy as np
from jax import lax
from jax.experimental import pallas as pl
from jax.experimental.pallas import tpu as pltpu
from jax.sharding import PartitionSpec as P

DEG = 7
N = DEG + 1
SWEEPS = 2
CHEB = 3
F32 = jnp.float32
BF16 = jnp.bfloat16
highest = lax.Precision.HIGHEST


def legendre_pair(points, degree):
    prev_poly = points * 0.0 + 1.0
    this_poly = points * 1.0
    for order in range(2, degree + 1):
        next_poly = ((2 * order - 1) * points * this_poly - (order - 1) * prev_poly) / order
        prev_poly = this_poly
        this_poly = next_poly
    return (this_poly, prev_poly)


def gll_tables(degree):
    count = degree + 1
    points = -np.cos(np.pi * np.arange(count) / degree)
    for newton_step in range(60):
        this_poly, prev_poly = legendre_pair(points, degree)
        points = points - (points * this_poly - prev_poly) / (count * this_poly)
    values, unused_poly = legendre_pair(points, degree)
    weights = 2.0 / (degree * (degree + 1) * values**2)
    identity_np = np.eye(count)
    spacing = points[:, None] - points[None, :] + identity_np
    derivative = values[:, None] / (values[None, :] * spacing) * (1.0 - identity_np)
    derivative[0, 0] = -degree * (degree + 1) / 4.0
    derivative[degree, degree] = degree * (degree + 1) / 4.0
    stiff_ratio = (weights[:, None] * derivative**2).sum(0) / weights
    return (weights, derivative, stiff_ratio)


WEIGHTS, DERIV, RATIO = gll_tables(DEG)


def halves(matrix):
    high = matrix.astype(BF16).astype(np.float32)
    low = matrix.astype(np.float32) - high
    return high, low


def z_matrices(blocks):
    width = blocks * N
    node = np.array([DEG * f + k for f in range(blocks) for k in range(N)])
    free = (node > 0) & (node < DEG * blocks)
    share = ((node[:, None] == node[None, :]) & free[:, None] & free[None, :]).astype(np.float64)
    grad = np.kron(np.eye(blocks), DERIV.T)
    back = np.kron(np.eye(blocks), DERIV) @ share
    zero = np.zeros((width, width))
    grad_hi, grad_lo = halves(grad)
    back_hi, back_lo = halves(back)
    w_grad = np.block([[grad_hi, grad_lo], [grad_hi, zero]])
    w_back = np.block([[back_hi, back_lo], [back_hi, zero]])
    w_share = np.concatenate([share, share], 0)
    return w_grad, w_back, w_share


def line_sums(vals, matrix, pairs=range(N // 2)):
    even = [vals[i] + vals[DEG - i] for i in range(N // 2)]
    odd = [vals[i] - vals[DEG - i] for i in range(N // 2)]
    outs = [None] * N
    for p in pairs:
        from_even = None
        from_odd = None
        for i in range(N // 2):
            te = float(np.float32((matrix[p, i] + matrix[p, DEG - i]) / 2.0)) * even[i]
            to = float(np.float32((matrix[p, i] - matrix[p, DEG - i]) / 2.0)) * odd[i]
            from_even = te if from_even is None else from_even + te
            from_odd = to if from_odd is None else from_odd + to
        outs[p] = from_odd + from_even
        outs[DEG - p] = from_odd - from_even
    return outs


def split_pair(value):
    high = value.astype(BF16)
    low = (value - high.astype(F32)).astype(BF16)
    return jnp.concatenate([high, low], axis=-1)


def dot(a, b):
    return jnp.dot(a, b, preferred_element_type=F32)


ROWS = 8
SIDE = 4
ORDER = (0, 3, 1, 2)
UNROLL = 2


def flip(value):
    return jnp.concatenate([value[SIDE:], value[:SIDE]], 0)


def whole(ref):
    return lambda c, i, j: ref[c, i, j]


def by_i(face_ref, inner_ref):
    return lambda c, i, j: face_ref[c, i // DEG, j] if i in (0, DEG) else inner_ref[c, i - 1, j]


def by_j(mid_ref, edge_ref):
    return lambda c, i, j: edge_ref[c, i, j // DEG] if j in (0, DEG) else mid_ref[c, i, j - 1]


def mixed(mid, full):
    return lambda c, i, j: full[c, i, j] if j in (0, DEG) else mid[c, i, j - 1]


def with_halo(src, xr_ref, yr_ref, face_at, c, i, j, tile):
    value = src[c, i, j]
    row = lax.broadcasted_iota(jnp.int32, (ROWS, 128), 0)
    if tile == 0 and i == DEG:
        face = xr_ref[face_at, j]
        value = jnp.where(row < SIDE, value, jnp.concatenate([face, face], 0))
    if isinstance(j, int) and j == DEG:
        face = yr_ref[face_at, i]
        first = jnp.broadcast_to(face[2 * tile : 2 * tile + 1], (ROWS, 128))
        second = jnp.broadcast_to(face[2 * tile + 1 : 2 * tile + 2], (ROWS, 128))
        value = jnp.where(row == SIDE - 1, first, jnp.where(row == ROWS - 1, second, value))
    return value


def received(ctl_ref, axis, even_ref, odd_ref, *at):
    is_even = ctl_ref[axis][:SIDE] < 0.5
    even = even_ref[at]
    odd = odd_ref[at]
    return jnp.where(is_even, even, odd), jnp.where(is_even, odd, even)


def sum_x(ctl_ref, xe_ref, xo_ref, parts, c, face_at, i, j, tile):
    total = parts[tile](c, i, j)
    if 0 < i < DEG:
        return total
    row = lax.broadcasted_iota(jnp.int32, (ROWS, 128), 0)
    across = DEG - i
    if tile == 0:
        right, left = received(ctl_ref, 0, xe_ref, xo_ref, face_at, j)
        face = right if i else left
        face = jnp.concatenate([face, face], 0)
        inner = parts[1](c, across, j)
        low, high = (inner, face) if i else (face, inner)
    else:
        middle = flip(parts[1](c, across, j))
        outer = parts[0](c, across, j)
        low, high = (middle, outer) if i else (outer, middle)
    return total + jnp.where(row < SIDE, low, high)


def sum_all(ctl_ref, faces, parts, c, face_at, i, j, tile):
    xe, xo, ye, yo = faces
    total = sum_x(ctl_ref, xe, xo, parts, c, face_at, i, j, tile)
    if isinstance(j, int) and j in (0, DEG):
        row = lax.broadcasted_iota(jnp.int32, (ROWS, 128), 0)
        top, bottom = received(ctl_ref, 1, ye, yo, face_at, i)
        face = top if j else bottom
        at = SIDE - 1 if j else 0
        first = jnp.broadcast_to(face[2 * tile : 2 * tile + 1], (ROWS, 128))
        second = jnp.broadcast_to(face[2 * tile + 1 : 2 * tile + 2], (ROWS, 128))
        total = total + jnp.where(row == at, first, jnp.where(row == SIDE + at, second, 0.0))
    return total


def loop(count, body, unroll=UNROLL):
    def inner(i, carry):
        body(i)
        return carry

    lax.fori_loop(0, count, inner, 0, unroll=unroll)


def gradients(planes, at, wg_ref, gx_ref, gz_ref):
    flat = jnp.concatenate([planes[c][i] for c in range(3) for i in range(N)], 0)
    both = dot(split_pair(flat), wg_ref[...])
    for c in range(3):
        outs = line_sums(planes[c], DERIV)
        for i in range(N):
            gx_ref[c, i, at] = outs[i]
    both = (both[:, :128] + both[:, 128:]).reshape(3, N, ROWS, 128)
    for c in range(3):
        for i in range(N):
            gz_ref[c, i, at] = both[c, i]


def stress(u_at, gx_at, gz_at, lam_ref, mu_ref, wb_ref, sx_ref, fz_ref, fy_ref):
    def plane(i):
        gy = [line_sums([u_at(c, i, j) for j in range(N)], DERIV) for c in range(3)]
        sy = [[None] * N for c in range(3)]
        sz = [[None] * N for c in range(3)]
        for j in range(N):
            gx = [gx_at(c, i, j) for c in range(3)]
            gz = [gz_at(c, i, j) for c in range(3)]
            mu = mu_ref[i, j]
            mu2 = mu + mu
            trace = lam_ref[i, j] * (gx[0] + gy[1][j] + gz[2])
            sxy = mu * (gx[1] + gy[0][j])
            sxz = mu * (gx[2] + gz[0])
            syz = mu * (gy[2][j] + gz[1])
            sx_ref[0, i, j] = mu2 * gx[0] + trace
            sx_ref[1, i, j] = sxy
            sx_ref[2, i, j] = sxz
            sz[0][j] = sxz
            sz[1][j] = syz
            sz[2][j] = mu2 * gz[2] + trace
            sy[0][j] = sxy
            sy[1][j] = mu2 * gy[1][j] + trace
            sy[2][j] = syz
        flat = jnp.concatenate([sz[c][j] for c in range(3) for j in range(N)], 0)
        both = dot(split_pair(flat), wb_ref[...])
        for c in range(3):
            outs = line_sums(sy[c], DERIV.T)
            for j in range(N):
                fy_ref[c, i, j] = outs[j]
        both = (both[:, :128] + both[:, 128:]).reshape(3, N, ROWS, 128)
        for c in range(3):
            fz_ref[c, i] = both[c]

    loop(N, plane)


def back(ws_ref, work, out_ref, nodes, planes):
    sx_ref, fz_ref, fy_ref = work
    pairs = sorted({min(i, DEG - i) for i in nodes})
    flat = []
    for j in planes:
        for c in range(3):
            outs = line_sums([sx_ref[c, i, j] for i in range(N)], DERIV.T, pairs)
            flat += [outs[i] + fy_ref[c, i, j] for i in nodes]
    both = dot(split_pair(jnp.concatenate(flat, 0)), ws_ref[...]).reshape(len(planes), 3, len(nodes), ROWS, 128)
    for at, j in enumerate(planes):
        for c in range(3):
            for k, i in enumerate(nodes):
                out_ref[c, k, j] = both[at, c, k] + fz_ref[c, i, j]


def back_loop(ws_ref, work, out_ref, nodes):
    loop(N, lambda j: back(ws_ref, work, out_ref, nodes, (j,)))


def join_y(part_ref):
    row = lax.broadcasted_iota(jnp.int32, (ROWS, 128), 0)
    near = row % SIDE

    def along(i):
        for c in range(3):
            last = part_ref[c, i, DEG]
            start = part_ref[c, i, 0]
            last = last + jnp.where(near < SIDE - 1, jnp.concatenate([start[1:], start[:1]], 0), 0.0)
            start = jnp.where(near > 0, jnp.concatenate([last[-1:], last[:-1]], 0), start)
            part_ref[c, i, DEG] = last
            part_ref[c, i, 0] = start

    loop(part_ref.shape[1], along)


def give_faces(ctl_ref, part_ref, first, xe_ref, xo_ref):
    is_even = ctl_ref[0][:SIDE] < 0.5
    end = part_ref.shape[1] - 1

    def plane(j):
        for c in range(3):
            right = part_ref[c, end, j][SIDE:]
            left = part_ref[c, 0, j][:SIDE]
            xe_ref[first + c, j] = jnp.where(is_even, right, left)
            xo_ref[first + c, j] = jnp.where(is_even, left, right)

    loop(N, plane)


ENDS = (0, DEG)
INSIDE = tuple(range(1, DEG))
ALL = tuple(range(N))


def send_first(ctl_ref, ws_ref, work, face_ref, xe_ref, xo_ref):
    back(ws_ref, work, face_ref, ENDS, ALL)
    join_y(face_ref)
    give_faces(ctl_ref, face_ref, 0, xe_ref, xo_ref)


def finish_second(ws_ref, work, work_0, inner_ref, au_ref):
    back_loop(ws_ref, work, au_ref, ALL)
    join_y(au_ref)
    back_loop(ws_ref, work_0, inner_ref, INSIDE)
    join_y(inner_ref)


def diag_kernel(lam_ref, mu_ref, ratio_ref, rk_ref, ws_ref, dg_ref):
    def diagonal(i):
        rows = [[None] * N for c in range(3)]
        for j in range(N):
            lam = lam_ref[i, j]
            mu = mu_ref[i, j]
            ri = ratio_ref[i]
            rk = rk_ref[...]
            total = rk + (ri + float(RATIO[j]))
            for c in range(3):
                own = (ri, float(RATIO[j]), rk)[c]
                rows[c][j] = lam * own + mu * (total + own)
        flat = jnp.concatenate([rows[c][j] for c in range(3) for j in range(N)], 0)
        both = dot(split_pair(flat), ws_ref[...]).reshape(3, N, ROWS, 128)
        for c in range(3):
            dg_ref[c, i] = both[c]

    loop(N, diagonal, 1)
    join_y(dg_ref)


def first_mid_kernel(wg_ref, xr_ref, t0_ref, t1_ref, *outs):
    for tile, src in enumerate((t0_ref, t1_ref)):
        u_out, gx_ref, gz_ref = outs[3 * tile : 3 * tile + 3]

        def plane(at):
            planes = [[with_halo(src, xr_ref, None, c, c, i, at + 1, tile) for i in range(N)] for c in range(3)]
            for c in range(3):
                for i in range(N):
                    u_out[c, i, at] = planes[c][i]
            gradients(planes, at, wg_ref, gx_ref, gz_ref)

        loop(N - 2, plane)


def first_kernel(tile, *refs):
    refs = list(refs)
    take = lambda count: [refs.pop(0) for _ in range(count)]
    ctl_ref, wg_ref, wb_ref, ws_ref, lam_ref, mu_ref, src, xr_ref, yr_ref, mid_ref, gx_ref, gz_ref = take(12)
    if tile == 0:
        (dg_ref,) = take(1)
        u_out, face_ref, xe_ref, xo_ref = take(4)
    else:
        work_0 = take(3)
        u_out, inner_ref, au_ref = take(3)
    work = take(3)
    sx_ref, fz_ref, fy_ref = work
    for k in range(2):
        planes = [[with_halo(src, xr_ref, yr_ref, c, c, i, DEG * k, tile) for i in range(N)] for c in range(3)]
        for c in range(3):
            for i in range(N):
                u_out[c, i, k] = planes[c][i]
        gradients(planes, DEG * k, wg_ref, sx_ref, fz_ref)
    stress(by_j(mid_ref, u_out), mixed(gx_ref, sx_ref), mixed(gz_ref, fz_ref), lam_ref, mu_ref, wb_ref, *work)
    if tile == 0:
        send_first(ctl_ref, ws_ref, work, face_ref, xe_ref, xo_ref)
        give_faces(ctl_ref, dg_ref, 3, xe_ref, xo_ref)
    else:
        finish_second(ws_ref, work, work_0, inner_ref, au_ref)


def corner_kernel(ctl_ref, xe_ref, xo_ref, face_ref, inner_ref, au_ref, *refs):
    ye_ref, yo_ref = refs[-2:]
    fields = [(by_i(face_ref, inner_ref), whole(au_ref))]
    if len(refs) > 2:
        fields.append((whole(refs[0]), whole(refs[1])))
    is_even = ctl_ref[1][:SIDE] < 0.5
    for n, parts in enumerate(fields):
        for c in range(3):
            at = 3 * n + c
            for i in range(N):
                rows_t = []
                rows_b = []
                for tile in range(2):
                    top = sum_x(ctl_ref, xe_ref, xo_ref, parts, c, at, i, DEG, tile)
                    bottom = sum_x(ctl_ref, xe_ref, xo_ref, parts, c, at, i, 0, tile)
                    rows_t += [top[SIDE - 1 : SIDE], top[-1:]]
                    rows_b += [bottom[:1], bottom[SIDE : SIDE + 1]]
                top = jnp.concatenate(rows_t, 0)
                bottom = jnp.concatenate(rows_b, 0)
                ye_ref[at, i] = jnp.where(is_even, top, bottom)
                yo_ref[at, i] = jnp.where(is_even, bottom, top)


def invert(diag):
    lane = lax.broadcasted_iota(jnp.int32, (ROWS, 128), 1)
    clamped = (lane == 0) | (lane == 127)
    return jnp.where(clamped, 0.0, 1.0 / jnp.where(clamped, 1.0, diag))


def advance(ctl_ref, stage, u, load, total, inv, change):
    change_new = ctl_ref[3 + 2 * stage] * (inv * (load - total))
    if stage:
        change_new = ctl_ref[2 + 2 * stage] * change + change_new
    return u + change_new, change_new


def mid_kernel(stage, with_diag, *refs):
    refs = list(refs)
    take = lambda count: [refs.pop(0) for _ in range(count)]
    ctl_ref, wg_ref, face_ref, inner_ref, au_ref, xe_ref, xo_ref = take(7)
    parts = (by_i(face_ref, inner_ref), whole(au_ref))
    diag_parts = [whole(ref) for ref in take(2)] if with_diag else None
    ins = []
    for tile in range(2):
        u_ref, b_ref = take(2)
        ins.append((u_ref, b_ref, None if with_diag else take(1)[0], take(1)[0] if stage else None))
    for tile in range(2):
        u_ref, b_ref, inv_ref, change_ref = ins[tile]
        u_out, gx_ref, gz_ref = take(3)
        change_out = take(1 if stage < CHEB - 1 else 0)
        inv_out = take(1)[0] if with_diag else None

        def plane(at):
            j = at + 1
            planes = [[None] * N for c in range(3)]
            for c in range(3):
                for i in range(N):
                    if with_diag:
                        inv = invert(sum_x(ctl_ref, xe_ref, xo_ref, diag_parts, c, 3 + c, i, j, tile))
                        inv_out[c, i, at] = inv
                    else:
                        inv = inv_ref[c, i, at]
                    total = sum_x(ctl_ref, xe_ref, xo_ref, parts, c, c, i, j, tile)
                    change = change_ref[c, i, at] if stage else None
                    planes[c][i], change = advance(ctl_ref, stage, u_ref[c, i, at], b_ref[c, i, j], total, inv, change)
                    if change_out:
                        change_out[0][c, i, at] = change
                    u_out[c, i, at] = planes[c][i]
            gradients(planes, at, wg_ref, gx_ref, gz_ref)

        loop(N - 2, plane)


def edge_kernel(tile, stage, with_diag, *refs):
    refs = list(refs)
    take = lambda count: [refs.pop(0) for _ in range(count)]
    ctl_ref, wg_ref, wb_ref, ws_ref, lam_ref, mu_ref, face_in, inner_in, au_in = take(9)
    faces = take(4)
    parts = (by_i(face_in, inner_in), whole(au_in))
    diag_parts = [whole(ref) for ref in take(2)] if with_diag else None
    mid_ref, gx_ref, gz_ref, u_ref, b_ref = take(5)
    inv_ref = None if with_diag else take(1)[0]
    change_ref = take(1)[0] if stage else None
    work_0 = take(3) if tile else None
    (u_out,) = take(1)
    change_out = take(1 if stage < CHEB - 1 else 0)
    inv_out = take(1)[0] if with_diag else None
    outs = take(2 if tile else 3)
    work = take(3)
    sx_ref, fz_ref, fy_ref = work
    for k in range(2):
        j = DEG * k
        planes = [[None] * N for c in range(3)]
        for c in range(3):
            for i in range(N):
                if with_diag:
                    inv = invert(sum_all(ctl_ref, faces, diag_parts, c, 3 + c, i, j, tile))
                    inv_out[c, i, k] = inv
                else:
                    inv = inv_ref[c, i, k]
                total = sum_all(ctl_ref, faces, parts, c, c, i, j, tile)
                change = change_ref[c, i, k] if stage else None
                planes[c][i], change = advance(ctl_ref, stage, u_ref[c, i, k], b_ref[c, i, j], total, inv, change)
                if change_out:
                    change_out[0][c, i, k] = change
                u_out[c, i, k] = planes[c][i]
        gradients(planes, j, wg_ref, sx_ref, fz_ref)

    stress(by_j(mid_ref, u_out), mixed(gx_ref, sx_ref), mixed(gz_ref, fz_ref), lam_ref, mu_ref, wb_ref, *work)
    if tile == 0:
        send_first(ctl_ref, ws_ref, work, *outs)
    else:
        finish_second(ws_ref, work, work_0, *outs)


def lane_pick(value, index):
    return jnp.take_along_axis(value, index, axis=1, mode="promise_in_bounds")


TILES = ((0, 8), (8, 16), (16, 24), (20, 28))


def load_kernel(ctl_ref, in_ref, t0_ref, t1_ref, xl_ref, yb_ref, work_ref):
    nodes_x, width = in_ref.shape[1], in_ref.shape[2]
    nodes_z = width // nodes_x
    outs = (t0_ref, t1_ref)
    lane = lax.broadcasted_iota(jnp.int32, (ROWS, 128), 1)
    node = DEG * (lane // N) + lane % N - 1
    free = (node >= 0) & (node < nodes_z)
    node = jnp.clip(node, 0, nodes_z - 1)
    zero = jnp.zeros((ROWS, 128), F32)
    for r in range(4):
        work_ref[nodes_x, pl.ds(8 * r, 8)] = zero

    def component(c, carry):
        for y in range(nodes_x):
            tile, shift = divmod(nodes_z * y, 128)
            at = node + shift
            begin = 128 * tile
            work_ref[y, pl.ds(24, 8)] = zero
            for low, high in TILES:
                here = in_ref[c, low:high, begin : begin + 128]
                got = lane_pick(here, at & 127)
                if shift + nodes_z > 128:
                    stop = min(begin + 256, width)
                    there = in_ref[c, low:high, begin + 128 : stop]
                    if stop < begin + 256:
                        there = jnp.concatenate([there, jnp.zeros((ROWS, begin + 256 - stop), F32)], 1)
                    got = jnp.where(at < 128, got, lane_pick(there, at & 127))
                work_ref[y, low:high] = jnp.where(free, got, 0.0)
        out_c = jnp.where(c == 2, 2, 1 - c)
        for i in range(N):
            for j in range(N):
                for which in range(2):
                    rows = [work_ref[DEG * ORDER[2 * which + k] + i, pl.ds(j, SIDE, stride=DEG)] for k in range(2)]
                    value = jnp.concatenate(rows, 0)
                    outs[which][out_c, i, j] = value
                    if j == 0:
                        yb_ref[out_c, i, pl.ds(2 * which, 1)] = value[:1]
                        yb_ref[out_c, i, pl.ds(2 * which + 1, 1)] = value[SIDE : SIDE + 1]
                    if i == 0 and which == 0:
                        xl_ref[out_c, j] = value[:SIDE]
        return carry

    lax.fori_loop(0, 3, component, 0)


def coeff_kernel(lame_ref, ctl_ref, material_ref, wz_ref, *outs):
    lane = lax.broadcasted_iota(jnp.int32, (ROWS, 128), 1)
    weight_z = wz_ref[...]
    for which in range(2):
        rows = [material_ref[b, ORDER[2 * which + k]][None] for k in range(2) for b in range(SIDE)]
        kind = jnp.concatenate(rows, 0).astype(F32)
        kind = jnp.concatenate([kind, jnp.zeros((ROWS, 128 - kind.shape[1]), F32)], 1)
        kind = lane_pick(kind, lane // N)
        for part in range(2):
            value = jnp.zeros((ROWS, 128), F32)
            for label in range(lame_ref.shape[1]):
                value = jnp.where(kind == float(label), lame_ref[part, label], value)
            value = value * weight_z
            for i in range(N):
                for j in range(N):
                    outs[2 * which + part][i, j] = value * float(WEIGHTS[i] * WEIGHTS[j])


def halo_corner_kernel(xr_ref, yb_ref, out_ref):
    row = lax.broadcasted_iota(jnp.int32, (SIDE, 128), 0)
    for n in range(6):
        for i in range(N):
            value = yb_ref[n, i]
            if i == DEG:
                value = jnp.where(row == 1, jnp.broadcast_to(xr_ref[n, 0][:1], (SIDE, 128)), value)
            out_ref[n, i] = value


def halo_kernel(xr_ref, yr_ref, t0_ref, t1_ref, o0_ref, o1_ref):
    for tile, (src, dst) in enumerate(((t0_ref, o0_ref), (t1_ref, o1_ref))):

        def plane(j):
            for c in range(3):
                for i in range(N):
                    dst[c, i, j] = with_halo(src, xr_ref, yr_ref, 3 + c, c, i, j, tile)

        plane(0)
        loop(N - 2, lambda at: plane(at + 1), 1)
        plane(DEG)


def store_kernel(with_residual, *refs):
    refs = list(refs)
    take = lambda count: [refs.pop(0) for _ in range(count)]
    if with_residual:
        ctl_ref, b0_ref, b1_ref, face_ref, inner_ref, au_ref = take(6)
        faces = take(4)
        sums = (by_i(face_ref, inner_ref), whole(au_ref))
        loads = (whole(b0_ref), whole(b1_ref))
        parts = [
            lambda c, i, j, tile=tile: loads[tile](c, i, j) - sum_all(ctl_ref, faces, sums, c, c, i, j, tile)
            for tile in range(2)
        ]
    else:
        parts = [by_j(*take(2)) for tile in range(2)]
    out_ref, work_ref = refs
    nodes_x, width = out_ref.shape[1], out_ref.shape[2]
    nodes_z = width // nodes_x
    lane = lax.broadcasted_iota(jnp.int32, (ROWS, 128), 1)

    def component(c, carry):
        in_c = jnp.where(c == 2, 2, 1 - c)
        for i in range(DEG):
            for j in range(DEG):
                for which in range(2):
                    value = parts[which](in_c, i, j)
                    for k in range(2):
                        at = DEG * ORDER[2 * which + k] + i
                        work_ref[at, pl.ds(j, SIDE, stride=DEG)] = value[SIDE * k : SIDE * k + SIDE]
        for begin in range(0, width, 128):
            stop = min(begin + 128, width)
            for low, high in TILES:
                result = None
                for y in range(begin // nodes_z, (stop - 1) // nodes_z + 1):
                    node = jnp.clip(lane + (begin - nodes_z * y), 0, nodes_z - 1) + 1
                    sevens = ((node.astype(F32) + 0.5) * (1.0 / DEG)).astype(jnp.int32)
                    got = lane_pick(work_ref[y, low:high], node + sevens)
                    result = got if result is None else jnp.where(lane + begin >= nodes_z * y, got, result)
                out_ref[c, low:high, begin:stop] = result[:, : stop - begin]
        return carry

    lax.fori_loop(0, 3, component, 0)


VM = pl.BlockSpec(memory_space=pltpu.VMEM)
SM = pl.BlockSpec(memory_space=pltpu.SMEM)
FIELD = (3, N, N, ROWS, 128)
MID = (3, N, N - 2, ROWS, 128)
EDGE = (3, N, 2, ROWS, 128)
FACE = (3, 2, N, ROWS, 128)
INNER = (3, N - 2, N, ROWS, 128)


def shape(dims):
    return jax.ShapeDtypeStruct(dims, F32)


def call(kernel, smem, inputs, outs, work=0, rows=FIELD):
    return pl.pallas_call(
        kernel,
        in_specs=[SM] * smem + [VM] * (len(inputs) - smem),
        out_specs=[VM] * len(outs),
        out_shape=[shape(dims) for dims in outs],
        scratch_shapes=[pltpu.VMEM(rows, F32)] * work,
        compiler_params=pltpu.CompilerParams(vmem_limit_bytes=6 << 20),
    )(*inputs)


def swaps(even, odd, axis):
    size = lax.axis_size(axis)
    got_odd = lax.ppermute(odd, axis, [(i, (((i + 1) ^ 1) - 1) % size) for i in range(size)])
    got_even = lax.ppermute(even, axis, [(i, i ^ 1) for i in range(size)])
    return got_even, got_odd


def exchange(ctl, x_faces, fields):
    xe, xo = swaps(*x_faces, "gy")
    ye, yo = call(corner_kernel, 0, (ctl, xe, xo, *fields), (xe.shape, xe.shape))
    ye, yo = swaps(ye, yo, "gx")
    return (xe, xo), (ye, yo)


def from_next(value, axis):
    size = lax.axis_size(axis)
    return lax.ppermute(value, axis, [(i, (i - 1) % size) for i in range(size)])


def local(right_side, guess, material, lame, upper, lower_ratio):
    elems_x, elems_y, elems_z = material.shape
    nodes_y = DEG * elems_y
    w_grad, w_back, w_share = z_matrices(elems_z)
    w_grad = jnp.asarray(w_grad, BF16)
    w_back = jnp.asarray(w_back, BF16)
    w_share = jnp.asarray(w_share, BF16)
    upper_edge = upper[0]
    lower_edge = lower_ratio[0] * upper_edge
    center = (upper_edge + lower_edge) / 2.0
    radius = (upper_edge - lower_edge) / 2.0
    sigma_ratio = center / radius
    pairs = [(jnp.zeros((), F32), 1.0 / center)]
    factor = 1.0 / sigma_ratio
    for step_index in range(CHEB - 1):
        factor_next = 1.0 / (2.0 * sigma_ratio - factor)
        pairs.append((factor_next * factor, 2.0 * factor_next / radius))
        factor = factor_next
    flags = [(lax.axis_index(axis) % 2).astype(F32) for axis in ("gy", "gx")]
    ctl = jnp.stack(flags + [value for pair in pairs for value in pair])
    ctl = jnp.broadcast_to(ctl[:, None, None], (2 + 2 * CHEB, ROWS, 128))
    grid = (N, N, ROWS, 128)
    weight_z = jnp.asarray(np.tile(WEIGHTS, (ROWS, elems_z)), F32)
    coeffs = call(coeff_kernel, 1, (lame, ctl, material, weight_z), (grid,) * 4)
    coeffs = [coeffs[:2], coeffs[2:]]

    plane = (3, N, SIDE, 128)
    staged = (nodes_y + 1, nodes_y + SIDE, 128)
    loads = [call(load_kernel, 0, (ctl, value), (FIELD, FIELD, plane, plane), 1, staged) for value in (guess, right_side)]
    x_halo = from_next(jnp.concatenate([load[2] for load in loads], 0), "gy")
    y_halo = jnp.concatenate([load[3] for load in loads], 0)
    (y_halo,) = call(halo_corner_kernel, 0, (x_halo, y_halo), (y_halo.shape,))
    y_halo = from_next(y_halo, "gx")
    ratio_z = jnp.asarray(np.tile(RATIO, (ROWS, elems_z)), F32)
    ratio_i = jnp.asarray(np.broadcast_to(RATIO[:, None, None], (N, ROWS, 128)), F32)
    weights = (w_grad, w_back, w_share)
    work = (FIELD,) * 3
    both_faces = ((6, N, SIDE, 128),) * 2
    diag = tuple(call(diag_kernel, 0, (*coeffs[tile], ratio_i, ratio_z, w_share), (FIELD,))[0] for tile in range(2))
    got = call(first_mid_kernel, 0, (w_grad, x_halo, *loads[0][:2]), (MID,) * 6)
    u_mid = [got[0], got[3]]

    def first(tile, extra, outs, scratch):
        inputs = (ctl, *weights, *coeffs[tile], loads[0][tile], x_halo, y_halo, *got[3 * tile : 3 * tile + 3], *extra)
        return call(lambda *refs: first_kernel(tile, *refs), 0, inputs, (EDGE,) + outs, scratch)

    edge_0, face, *rest = first(0, diag[:1], (FACE, *both_faces, *work), 0)
    x_faces, work_0 = rest[:2], rest[2:]
    edge_1, inner, au = first(1, work_0, (INNER, FIELD), 3)
    u_edge = [edge_0, edge_1]
    b = call(halo_kernel, 0, (x_halo, y_halo, *loads[1][:2]), (FIELD, FIELD))
    change_mid = [None, None]
    change_edge = [None, None]
    inv_mid = [None, None]
    inv_edge = [None, None]
    for count in range(SWEEPS * CHEB):
        stage = count % CHEB
        with_diag = count == 0
        sums = (face, inner, au)
        x_got, y_got = exchange(ctl, x_faces, sums + (diag if with_diag else ()))
        keep_inv = 1 if with_diag else 0

        inputs = (ctl, w_grad, *sums, *x_got) + (diag if with_diag else ())
        for tile in range(2):
            inputs += (u_mid[tile], b[tile]) + (() if with_diag else (inv_mid[tile],))
            inputs += (change_mid[tile],) if stage else ()
        keep_change = 1 if stage < CHEB - 1 else 0
        each = 3 + keep_change + keep_inv
        outs = (MID,) * each * 2
        results = call(lambda *refs: mid_kernel(stage, with_diag, *refs), 0, inputs, outs)
        slopes = [None, None]
        for tile in range(2):
            got = results[each * tile : each * (tile + 1)]
            u_mid[tile] = got[0]
            slopes[tile] = got[1:3]
            if keep_change:
                change_mid[tile] = got[3]
            if with_diag:
                inv_mid[tile] = got[-1]

        for tile in range(2):
            inputs = (ctl, *weights, *coeffs[tile], *sums, *x_got, *y_got) + (diag if with_diag else ())
            inputs += (u_mid[tile], *slopes[tile], u_edge[tile], b[tile])
            inputs += () if with_diag else (inv_edge[tile],)
            inputs += (change_edge[tile],) if stage else ()
            inputs += tuple(work_0) if tile else ()
            outs = (EDGE,) * (1 + keep_change + keep_inv)
            outs += (INNER, FIELD) if tile else (FACE, *((3, N, SIDE, 128),) * 2, *work)
            results = list(
                call(lambda *refs: edge_kernel(tile, stage, with_diag, *refs), 0, inputs, outs, 3 if tile else 0)
            )
            u_edge[tile] = results.pop(0)
            if keep_change:
                change_edge[tile] = results.pop(0)
            if with_diag:
                inv_edge[tile] = results.pop(0)
            if tile:
                inner, au = results
            else:
                face, x_faces, work_0 = results[0], results[1:3], results[3:]
    sums = (face, inner, au)
    x_got, y_got = exchange(ctl, x_faces, sums)

    def store(with_residual, inputs):
        return call(lambda *refs: store_kernel(with_residual, *refs), 0, inputs, (guess.shape,), 1, staged)[0]

    smoothed = store(False, (u_mid[0], u_edge[0], u_mid[1], u_edge[1]))
    return (smoothed, store(True, (ctl, *b, *sums, *x_got, *y_got)))


def solution(mesh):
    placed = (P(None, "gx", "gy"), P(None, "gx", "gy"), P("gx", "gy", None), P(), P(), P())
    return jax.shard_map(
        local,
        mesh=mesh,
        in_specs=placed,
        out_specs=(P(None, "gx", "gy"), P(None, "gx", "gy")),
        check_vma=False,
    )
```

```python
import jax
import jax.numpy as jnp
import numpy as np
from jax import lax
from jax.experimental import pallas as pl
from jax.experimental.pallas import tpu as pltpu
from jax.sharding import PartitionSpec as P

DEG = 7
N = DEG + 1
SWEEPS = 2
CHEB = 3
F32 = jnp.float32
BF16 = jnp.bfloat16
highest = lax.Precision.HIGHEST


def legendre_pair(points, degree):
    prev_poly = points * 0.0 + 1.0
    this_poly = points * 1.0
    for order in range(2, degree + 1):
        next_poly = ((2 * order - 1) * points * this_poly - (order - 1) * prev_poly) / order
        prev_poly = this_poly
        this_poly = next_poly
    return (this_poly, prev_poly)


def gll_tables(degree):
    count = degree + 1
    points = -np.cos(np.pi * np.arange(count) / degree)
    for newton_step in range(60):
        this_poly, prev_poly = legendre_pair(points, degree)
        points = points - (points * this_poly - prev_poly) / (count * this_poly)
    values, unused_poly = legendre_pair(points, degree)
    weights = 2.0 / (degree * (degree + 1) * values**2)
    identity_np = np.eye(count)
    spacing = points[:, None] - points[None, :] + identity_np
    derivative = values[:, None] / (values[None, :] * spacing) * (1.0 - identity_np)
    derivative[0, 0] = -degree * (degree + 1) / 4.0
    derivative[degree, degree] = degree * (degree + 1) / 4.0
    stiff_ratio = (weights[:, None] * derivative**2).sum(0) / weights
    return (weights, derivative, stiff_ratio)


WEIGHTS, DERIV, RATIO = gll_tables(DEG)


def halves(matrix):
    high = matrix.astype(BF16).astype(np.float32)
    low = matrix.astype(np.float32) - high
    return high, low


def z_matrices(blocks):
    width = blocks * N
    node = np.array([DEG * f + k for f in range(blocks) for k in range(N)])
    free = (node > 0) & (node < DEG * blocks)
    share = ((node[:, None] == node[None, :]) & free[:, None] & free[None, :]).astype(np.float64)
    grad = np.kron(np.eye(blocks), DERIV.T)
    back = np.kron(np.eye(blocks), DERIV) @ share
    zero = np.zeros((width, width))
    grad_hi, grad_lo = halves(grad)
    back_hi, back_lo = halves(back)
    w_grad = np.block([[grad_hi, grad_lo], [grad_hi, zero]])
    w_back = np.block([[back_hi, back_lo], [back_hi, zero]])
    w_share = np.concatenate([share, share], 0)
    return w_grad, w_back, w_share


def line_sums(vals, matrix, pairs=range(N // 2)):
    even = [vals[i] + vals[DEG - i] for i in range(N // 2)]
    odd = [vals[i] - vals[DEG - i] for i in range(N // 2)]
    outs = [None] * N
    for p in pairs:
        from_even = None
        from_odd = None
        for i in range(N // 2):
            te = float(np.float32((matrix[p, i] + matrix[p, DEG - i]) / 2.0)) * even[i]
            to = float(np.float32((matrix[p, i] - matrix[p, DEG - i]) / 2.0)) * odd[i]
            from_even = te if from_even is None else from_even + te
            from_odd = to if from_odd is None else from_odd + to
        outs[p] = from_odd + from_even
        outs[DEG - p] = from_odd - from_even
    return outs


def pair_terms(low, high, matrix, i, p):
    even = float(np.float32((matrix[p, i] + matrix[p, DEG - i]) / 2.0)) * (low + high)
    odd = float(np.float32((matrix[p, i] - matrix[p, DEG - i]) / 2.0)) * (low - high)
    return even, odd


def inner_sums(vals, matrix):
    outs = [None] * N
    for p in range(N // 2):
        terms = [pair_terms(vals[i - 1], vals[DEG - i - 1], matrix, i, p) for i in range(1, N // 2)]
        from_even = terms[0][0] + terms[1][0] + terms[2][0]
        from_odd = terms[0][1] + terms[1][1] + terms[2][1]
        outs[p] = from_odd + from_even
        outs[DEG - p] = from_odd - from_even
    return outs


def add_ends(partial, low, high, matrix):
    outs = [None] * N
    for p in range(N // 2):
        from_even, from_odd = pair_terms(low, high, matrix, 0, p)
        outs[p] = partial[p] + (from_odd + from_even)
        outs[DEG - p] = partial[DEG - p] + (from_odd - from_even)
    return outs


def split_pair(value):
    high = value.astype(BF16)
    low = (value - high.astype(F32)).astype(BF16)
    return jnp.concatenate([high, low], axis=-1)


def dot(a, b):
    return jnp.dot(a, b, preferred_element_type=F32)


ROWS = 8
SIDE = 4
ORDER = (0, 3, 1, 2)
UNROLL = 2


def flip(value):
    return jnp.concatenate([value[SIDE:], value[:SIDE]], 0)


def whole(ref):
    return lambda c, i, j: ref[c, i, j]


def by_i(face_ref, inner_ref):
    return lambda c, i, j: face_ref[c, i // DEG, j] if i in (0, DEG) else inner_ref[c, i - 1, j]


def by_j(mid_ref, edge_ref):
    return lambda c, i, j: edge_ref[c, i, j // DEG] if j in (0, DEG) else mid_ref[c, i, j - 1]


def mixed(mid, full):
    return lambda c, i, j: full[c, i, j] if j in (0, DEG) else mid[c, i, j - 1]


def with_halo(src, xr_ref, yr_ref, face_at, c, i, j, tile):
    value = src[c, i, j]
    row = lax.broadcasted_iota(jnp.int32, (ROWS, 128), 0)
    if tile == 0 and i == DEG:
        face = xr_ref[face_at, j]
        value = jnp.where(row < SIDE, value, jnp.concatenate([face, face], 0))
    if isinstance(j, int) and j == DEG:
        face = yr_ref[face_at, i]
        first = jnp.broadcast_to(face[2 * tile : 2 * tile + 1], (ROWS, 128))
        second = jnp.broadcast_to(face[2 * tile + 1 : 2 * tile + 2], (ROWS, 128))
        value = jnp.where(row == SIDE - 1, first, jnp.where(row == ROWS - 1, second, value))
    return value


def received(ctl_ref, axis, even_ref, odd_ref, *at):
    is_even = ctl_ref[axis][:SIDE] < 0.5
    even = even_ref[at]
    odd = odd_ref[at]
    return jnp.where(is_even, even, odd), jnp.where(is_even, odd, even)


def sum_x(ctl_ref, xe_ref, xo_ref, parts, c, face_at, i, j, tile):
    total = parts[tile](c, i, j)
    if 0 < i < DEG:
        return total
    row = lax.broadcasted_iota(jnp.int32, (ROWS, 128), 0)
    across = DEG - i
    if tile == 0:
        right, left = received(ctl_ref, 0, xe_ref, xo_ref, face_at, j)
        face = right if i else left
        face = jnp.concatenate([face, face], 0)
        inner = parts[1](c, across, j)
        low, high = (inner, face) if i else (face, inner)
    else:
        middle = flip(parts[1](c, across, j))
        outer = parts[0](c, across, j)
        low, high = (middle, outer) if i else (outer, middle)
    return total + jnp.where(row < SIDE, low, high)


def sum_all(ctl_ref, faces, parts, c, face_at, i, j, tile):
    xe, xo, ye, yo = faces
    total = sum_x(ctl_ref, xe, xo, parts, c, face_at, i, j, tile)
    if isinstance(j, int) and j in (0, DEG):
        row = lax.broadcasted_iota(jnp.int32, (ROWS, 128), 0)
        top, bottom = received(ctl_ref, 1, ye, yo, face_at, i)
        face = top if j else bottom
        at = SIDE - 1 if j else 0
        first = jnp.broadcast_to(face[2 * tile : 2 * tile + 1], (ROWS, 128))
        second = jnp.broadcast_to(face[2 * tile + 1 : 2 * tile + 2], (ROWS, 128))
        total = total + jnp.where(row == at, first, jnp.where(row == SIDE + at, second, 0.0))
    return total


def loop(count, body, unroll=UNROLL):
    def inner(i, carry):
        body(i)
        return carry

    lax.fori_loop(0, count, inner, 0, unroll=unroll)


def gradients(planes, at, wg_ref, gx_ref, gz_ref):
    flat = jnp.concatenate([planes[c][i] for c in range(3) for i in range(N)], 0)
    both = dot(split_pair(flat), wg_ref[...])
    for c in range(3):
        outs = line_sums(planes[c], DERIV)
        for i in range(N):
            gx_ref[c, i, at] = outs[i]
    both = (both[:, :128] + both[:, 128:]).reshape(3, N, ROWS, 128)
    for c in range(3):
        for i in range(N):
            gz_ref[c, i, at] = both[c, i]


def inner_slopes(u_ref, gy_ref):
    def plane(i):
        for c in range(3):
            outs = inner_sums([u_ref[c, i, at] for at in range(N - 2)], DERIV)
            for j in range(N):
                gy_ref[c, i, j] = outs[j]

    loop(N, plane)


def back_yz(sy, sz, i, wb_ref, fz_ref, fy_ref):
    flat = jnp.concatenate([sz[c][j] for c in range(3) for j in range(N)], 0)
    both = dot(split_pair(flat), wb_ref[...])
    for c in range(3):
        outs = line_sums(sy[c], DERIV.T)
        for j in range(N):
            fy_ref[c, i, j] = outs[j]
    both = (both[:, :128] + both[:, 128:]).reshape(3, N, ROWS, 128)
    for c in range(3):
        fz_ref[c, i] = both[c]


def stress(tile, edge_ref, gy_ref, gx_at, gz_at, lam_ref, mu_ref, wb_ref, sx_ref, fz_ref, fy_ref):
    def plane(i, later=False):
        gy = [
            add_ends([gy_ref[c, i, j] for j in range(N)], edge_ref[c, i, 0], edge_ref[c, i, 1], DERIV)
            for c in range(3)
        ]
        sy = [[None] * N for c in range(3)]
        sz = [[None] * N for c in range(3)]
        for j in range(N):
            gx = [gx_at(c, i, j) for c in range(3)]
            gz = [gz_at(c, i, j) for c in range(3)]
            mu = mu_ref[i, j]
            mu2 = mu + mu
            trace = lam_ref[i, j] * (gx[0] + gy[1][j] + gz[2])
            sxy = mu * (gx[1] + gy[0][j])
            sxz = mu * (gx[2] + gz[0])
            syz = mu * (gy[2][j] + gz[1])
            sx_ref[0, i, j] = mu2 * gx[0] + trace
            sx_ref[1, i, j] = sxy
            sx_ref[2, i, j] = sxz
            sz[0][j] = sxz
            sz[1][j] = syz
            sz[2][j] = mu2 * gz[2] + trace
            sy[0][j] = sxy
            sy[1][j] = mu2 * gy[1][j] + trace
            sy[2][j] = syz
            if later:
                fy_ref[1, i, j] = sy[1][j]
                fy_ref[2, i, j] = syz
                fz_ref[2, i, j] = sz[2][j]
        if not later:
            back_yz(sy, sz, i, wb_ref, fz_ref, fy_ref)

    if tile:
        loop(N, plane)
    else:
        plane(0)
        plane(DEG)
        loop(N - 2, lambda at: plane(at + 1, True))


def late_back(wb_ref, work_0, fz_ref, fy_ref):
    sx_ref, sz_ref, sy_ref = work_0

    def plane(at):
        i = at + 1
        sxy = [sx_ref[1, i, j] for j in range(N)]
        sxz = [sx_ref[2, i, j] for j in range(N)]
        syy = [sy_ref[1, i, j] for j in range(N)]
        syz = [sy_ref[2, i, j] for j in range(N)]
        szz = [sz_ref[2, i, j] for j in range(N)]
        back_yz((sxy, syy, syz), (sxz, syz, szz), i, wb_ref, fz_ref, fy_ref)

    loop(N - 2, plane)


def back(ws_ref, work, out_ref, nodes, planes):
    sx_ref, fz_ref, fy_ref = work
    pairs = sorted({min(i, DEG - i) for i in nodes})
    flat = []
    for j in planes:
        for c in range(3):
            outs = line_sums([sx_ref[c, i, j] for i in range(N)], DERIV.T, pairs)
            flat += [outs[i] + fy_ref[c, i, j] for i in nodes]
    both = dot(split_pair(jnp.concatenate(flat, 0)), ws_ref[...]).reshape(len(planes), 3, len(nodes), ROWS, 128)
    for at, j in enumerate(planes):
        for c in range(3):
            for k, i in enumerate(nodes):
                out_ref[c, k, j] = both[at, c, k] + fz_ref[c, i, j]


def back_loop(ws_ref, work, out_ref, nodes):
    loop(N, lambda j: back(ws_ref, work, out_ref, nodes, (j,)))


def join_y(part_ref):
    row = lax.broadcasted_iota(jnp.int32, (ROWS, 128), 0)
    near = row % SIDE

    def along(i):
        for c in range(3):
            last = part_ref[c, i, DEG]
            start = part_ref[c, i, 0]
            last = last + jnp.where(near < SIDE - 1, jnp.concatenate([start[1:], start[:1]], 0), 0.0)
            start = jnp.where(near > 0, jnp.concatenate([last[-1:], last[:-1]], 0), start)
            part_ref[c, i, DEG] = last
            part_ref[c, i, 0] = start

    loop(part_ref.shape[1], along)


def give_faces(ctl_ref, part_ref, first, xe_ref, xo_ref):
    is_even = ctl_ref[0][:SIDE] < 0.5
    end = part_ref.shape[1] - 1

    def plane(j):
        for c in range(3):
            right = part_ref[c, end, j][SIDE:]
            left = part_ref[c, 0, j][:SIDE]
            xe_ref[first + c, j] = jnp.where(is_even, right, left)
            xo_ref[first + c, j] = jnp.where(is_even, left, right)

    loop(N, plane)


ENDS = (0, DEG)
INSIDE = tuple(range(1, DEG))
ALL = tuple(range(N))


def send_first(ctl_ref, ws_ref, work, face_ref, xe_ref, xo_ref):
    back(ws_ref, work, face_ref, ENDS, ALL)
    join_y(face_ref)
    give_faces(ctl_ref, face_ref, 0, xe_ref, xo_ref)


def finish_second(wb_ref, ws_ref, work, work_0, inner_ref, au_ref):
    back_loop(ws_ref, work, au_ref, ALL)
    join_y(au_ref)
    sx_ref, fz_ref, fy_ref = work
    late_back(wb_ref, work_0, fz_ref, fy_ref)
    back_loop(ws_ref, (work_0[0], fz_ref, fy_ref), inner_ref, INSIDE)
    join_y(inner_ref)


def diag_kernel(lam_ref, mu_ref, ratio_ref, rk_ref, ws_ref, dg_ref):
    def diagonal(i):
        rows = [[None] * N for c in range(3)]
        for j in range(N):
            lam = lam_ref[i, j]
            mu = mu_ref[i, j]
            ri = ratio_ref[i]
            rk = rk_ref[...]
            total = rk + (ri + float(RATIO[j]))
            for c in range(3):
                own = (ri, float(RATIO[j]), rk)[c]
                rows[c][j] = lam * own + mu * (total + own)
        flat = jnp.concatenate([rows[c][j] for c in range(3) for j in range(N)], 0)
        both = dot(split_pair(flat), ws_ref[...]).reshape(3, N, ROWS, 128)
        for c in range(3):
            dg_ref[c, i] = both[c]

    loop(N, diagonal, 1)
    join_y(dg_ref)


def first_mid_kernel(wg_ref, xr_ref, t0_ref, t1_ref, *outs):
    for tile, src in enumerate((t0_ref, t1_ref)):
        u_out, gx_ref, gz_ref, gy_ref = outs[4 * tile : 4 * tile + 4]

        def plane(at):
            planes = [[with_halo(src, xr_ref, None, c, c, i, at + 1, tile) for i in range(N)] for c in range(3)]
            for c in range(3):
                for i in range(N):
                    u_out[c, i, at] = planes[c][i]
            gradients(planes, at, wg_ref, gx_ref, gz_ref)

        loop(N - 2, plane)
        inner_slopes(u_out, gy_ref)


def first_kernel(tile, *refs):
    refs = list(refs)
    take = lambda count: [refs.pop(0) for _ in range(count)]
    ctl_ref, wg_ref, wb_ref, ws_ref, lam_ref, mu_ref, src, xr_ref, yr_ref, gx_ref, gz_ref, gy_ref = take(12)
    if tile == 0:
        (dg_ref,) = take(1)
        u_out, face_ref, xe_ref, xo_ref = take(4)
    else:
        work_0 = take(3)
        u_out, inner_ref, au_ref = take(3)
    work = take(3)
    sx_ref, fz_ref, fy_ref = work
    for k in range(2):
        planes = [[with_halo(src, xr_ref, yr_ref, c, c, i, DEG * k, tile) for i in range(N)] for c in range(3)]
        for c in range(3):
            for i in range(N):
                u_out[c, i, k] = planes[c][i]
        gradients(planes, DEG * k, wg_ref, sx_ref, fz_ref)
    stress(tile, u_out, gy_ref, mixed(gx_ref, sx_ref), mixed(gz_ref, fz_ref), lam_ref, mu_ref, wb_ref, *work)
    if tile == 0:
        send_first(ctl_ref, ws_ref, work, face_ref, xe_ref, xo_ref)
        give_faces(ctl_ref, dg_ref, 3, xe_ref, xo_ref)
    else:
        finish_second(wb_ref, ws_ref, work, work_0, inner_ref, au_ref)


def corner_kernel(ctl_ref, xe_ref, xo_ref, face_ref, inner_ref, au_ref, *refs):
    ye_ref, yo_ref = refs[-2:]
    fields = [(by_i(face_ref, inner_ref), whole(au_ref))]
    if len(refs) > 2:
        fields.append((whole(refs[0]), whole(refs[1])))
    is_even = ctl_ref[1][:SIDE] < 0.5
    for n, parts in enumerate(fields):
        for c in range(3):
            at = 3 * n + c
            for i in range(N):
                rows_t = []
                rows_b = []
                for tile in range(2):
                    top = sum_x(ctl_ref, xe_ref, xo_ref, parts, c, at, i, DEG, tile)
                    bottom = sum_x(ctl_ref, xe_ref, xo_ref, parts, c, at, i, 0, tile)
                    rows_t += [top[SIDE - 1 : SIDE], top[-1:]]
                    rows_b += [bottom[:1], bottom[SIDE : SIDE + 1]]
                top = jnp.concatenate(rows_t, 0)
                bottom = jnp.concatenate(rows_b, 0)
                ye_ref[at, i] = jnp.where(is_even, top, bottom)
                yo_ref[at, i] = jnp.where(is_even, bottom, top)


def invert(diag):
    lane = lax.broadcasted_iota(jnp.int32, (ROWS, 128), 1)
    clamped = (lane == 0) | (lane == 127)
    return jnp.where(clamped, 0.0, 1.0 / jnp.where(clamped, 1.0, diag))


def advance(ctl_ref, stage, u, load, total, inv, change):
    change_new = ctl_ref[3 + 2 * stage] * (inv * (load - total))
    if stage:
        change_new = ctl_ref[2 + 2 * stage] * change + change_new
    return u + change_new, change_new


def mid_kernel(stage, with_diag, *refs):
    refs = list(refs)
    take = lambda count: [refs.pop(0) for _ in range(count)]
    ctl_ref, wg_ref, face_ref, inner_ref, au_ref, xe_ref, xo_ref = take(7)
    parts = (by_i(face_ref, inner_ref), whole(au_ref))
    diag_parts = [whole(ref) for ref in take(2)] if with_diag else None
    ins = []
    for tile in range(2):
        u_ref, b_ref = take(2)
        ins.append((u_ref, b_ref, None if with_diag else take(1)[0], take(1)[0] if stage else None))
    for tile in range(2):
        u_ref, b_ref, inv_ref, change_ref = ins[tile]
        u_out, gx_ref, gz_ref, gy_ref = take(4)
        change_out = take(1 if stage < CHEB - 1 else 0)
        inv_out = take(1)[0] if with_diag else None

        def plane(at):
            j = at + 1
            planes = [[None] * N for c in range(3)]
            for c in range(3):
                for i in range(N):
                    if with_diag:
                        inv = invert(sum_x(ctl_ref, xe_ref, xo_ref, diag_parts, c, 3 + c, i, j, tile))
                        inv_out[c, i, at] = inv
                    else:
                        inv = inv_ref[c, i, at]
                    total = sum_x(ctl_ref, xe_ref, xo_ref, parts, c, c, i, j, tile)
                    change = change_ref[c, i, at] if stage else None
                    planes[c][i], change = advance(ctl_ref, stage, u_ref[c, i, at], b_ref[c, i, j], total, inv, change)
                    if change_out:
                        change_out[0][c, i, at] = change
                    u_out[c, i, at] = planes[c][i]
            gradients(planes, at, wg_ref, gx_ref, gz_ref)

        loop(N - 2, plane)
        inner_slopes(u_out, gy_ref)


def edge_kernel(tile, stage, with_diag, *refs):
    refs = list(refs)
    take = lambda count: [refs.pop(0) for _ in range(count)]
    ctl_ref, wg_ref, wb_ref, ws_ref, lam_ref, mu_ref, face_in, inner_in, au_in = take(9)
    faces = take(4)
    parts = (by_i(face_in, inner_in), whole(au_in))
    diag_parts = [whole(ref) for ref in take(2)] if with_diag else None
    gx_ref, gz_ref, gy_ref, u_ref, b_ref = take(5)
    inv_ref = None if with_diag else take(1)[0]
    change_ref = take(1)[0] if stage else None
    work_0 = take(3) if tile else None
    (u_out,) = take(1)
    change_out = take(1 if stage < CHEB - 1 else 0)
    inv_out = take(1)[0] if with_diag else None
    outs = take(2 if tile else 3)
    work = take(3)
    sx_ref, fz_ref, fy_ref = work
    for k in range(2):
        j = DEG * k
        planes = [[None] * N for c in range(3)]
        for c in range(3):
            for i in range(N):
                if with_diag:
                    inv = invert(sum_all(ctl_ref, faces, diag_parts, c, 3 + c, i, j, tile))
                    inv_out[c, i, k] = inv
                else:
                    inv = inv_ref[c, i, k]
                total = sum_all(ctl_ref, faces, parts, c, c, i, j, tile)
                change = change_ref[c, i, k] if stage else None
                planes[c][i], change = advance(ctl_ref, stage, u_ref[c, i, k], b_ref[c, i, j], total, inv, change)
                if change_out:
                    change_out[0][c, i, k] = change
                u_out[c, i, k] = planes[c][i]
        gradients(planes, j, wg_ref, sx_ref, fz_ref)

    stress(tile, u_out, gy_ref, mixed(gx_ref, sx_ref), mixed(gz_ref, fz_ref), lam_ref, mu_ref, wb_ref, *work)
    if tile == 0:
        send_first(ctl_ref, ws_ref, work, *outs)
    else:
        finish_second(wb_ref, ws_ref, work, work_0, *outs)


def lane_pick(value, index):
    return jnp.take_along_axis(value, index, axis=1, mode="promise_in_bounds")


TILES = ((0, 8), (8, 16), (16, 24), (20, 28))


def load_kernel(ctl_ref, in_ref, t0_ref, t1_ref, xl_ref, yb_ref, work_ref):
    nodes_x, width = in_ref.shape[1], in_ref.shape[2]
    nodes_z = width // nodes_x
    outs = (t0_ref, t1_ref)
    lane = lax.broadcasted_iota(jnp.int32, (ROWS, 128), 1)
    node = DEG * (lane // N) + lane % N - 1
    free = (node >= 0) & (node < nodes_z)
    node = jnp.clip(node, 0, nodes_z - 1)
    zero = jnp.zeros((ROWS, 128), F32)
    for r in range(4):
        work_ref[nodes_x, pl.ds(8 * r, 8)] = zero

    def component(c, carry):
        for y in range(nodes_x):
            tile, shift = divmod(nodes_z * y, 128)
            at = node + shift
            begin = 128 * tile
            work_ref[y, pl.ds(24, 8)] = zero
            for low, high in TILES:
                here = in_ref[c, low:high, begin : begin + 128]
                got = lane_pick(here, at & 127)
                if shift + nodes_z > 128:
                    stop = min(begin + 256, width)
                    there = in_ref[c, low:high, begin + 128 : stop]
                    if stop < begin + 256:
                        there = jnp.concatenate([there, jnp.zeros((ROWS, begin + 256 - stop), F32)], 1)
                    got = jnp.where(at < 128, got, lane_pick(there, at & 127))
                work_ref[y, low:high] = jnp.where(free, got, 0.0)
        out_c = jnp.where(c == 2, 2, 1 - c)
        for i in range(N):
            for j in range(N):
                for which in range(2):
                    rows = [work_ref[DEG * ORDER[2 * which + k] + i, pl.ds(j, SIDE, stride=DEG)] for k in range(2)]
                    value = jnp.concatenate(rows, 0)
                    outs[which][out_c, i, j] = value
                    if j == 0:
                        yb_ref[out_c, i, pl.ds(2 * which, 1)] = value[:1]
                        yb_ref[out_c, i, pl.ds(2 * which + 1, 1)] = value[SIDE : SIDE + 1]
                    if i == 0 and which == 0:
                        xl_ref[out_c, j] = value[:SIDE]
        return carry

    lax.fori_loop(0, 3, component, 0)


def coeff_kernel(lame_ref, ctl_ref, material_ref, wz_ref, *outs):
    lane = lax.broadcasted_iota(jnp.int32, (ROWS, 128), 1)
    weight_z = wz_ref[...]
    for which in range(2):
        rows = [material_ref[b, ORDER[2 * which + k]][None] for k in range(2) for b in range(SIDE)]
        kind = jnp.concatenate(rows, 0).astype(F32)
        kind = jnp.concatenate([kind, jnp.zeros((ROWS, 128 - kind.shape[1]), F32)], 1)
        kind = lane_pick(kind, lane // N)
        for part in range(2):
            value = jnp.zeros((ROWS, 128), F32)
            for label in range(lame_ref.shape[1]):
                value = jnp.where(kind == float(label), lame_ref[part, label], value)
            value = value * weight_z
            for i in range(N):
                for j in range(N):
                    outs[2 * which + part][i, j] = value * float(WEIGHTS[i] * WEIGHTS[j])


def halo_corner_kernel(xr_ref, yb_ref, out_ref):
    row = lax.broadcasted_iota(jnp.int32, (SIDE, 128), 0)
    for n in range(6):
        for i in range(N):
            value = yb_ref[n, i]
            if i == DEG:
                value = jnp.where(row == 1, jnp.broadcast_to(xr_ref[n, 0][:1], (SIDE, 128)), value)
            out_ref[n, i] = value


def halo_kernel(xr_ref, yr_ref, t0_ref, t1_ref, o0_ref, o1_ref):
    for tile, (src, dst) in enumerate(((t0_ref, o0_ref), (t1_ref, o1_ref))):

        def plane(j):
            for c in range(3):
                for i in range(N):
                    dst[c, i, j] = with_halo(src, xr_ref, yr_ref, 3 + c, c, i, j, tile)

        plane(0)
        loop(N - 2, lambda at: plane(at + 1), 1)
        plane(DEG)


def store_kernel(with_residual, *refs):
    refs = list(refs)
    take = lambda count: [refs.pop(0) for _ in range(count)]
    if with_residual:
        ctl_ref, b0_ref, b1_ref, face_ref, inner_ref, au_ref = take(6)
        faces = take(4)
        sums = (by_i(face_ref, inner_ref), whole(au_ref))
        loads = (whole(b0_ref), whole(b1_ref))
        parts = [
            lambda c, i, j, tile=tile: loads[tile](c, i, j) - sum_all(ctl_ref, faces, sums, c, c, i, j, tile)
            for tile in range(2)
        ]
    else:
        parts = [by_j(*take(2)) for tile in range(2)]
    out_ref, work_ref = refs
    nodes_x, width = out_ref.shape[1], out_ref.shape[2]
    nodes_z = width // nodes_x
    lane = lax.broadcasted_iota(jnp.int32, (ROWS, 128), 1)

    def component(c, carry):
        in_c = jnp.where(c == 2, 2, 1 - c)
        for i in range(DEG):
            for j in range(DEG):
                for which in range(2):
                    value = parts[which](in_c, i, j)
                    for k in range(2):
                        at = DEG * ORDER[2 * which + k] + i
                        work_ref[at, pl.ds(j, SIDE, stride=DEG)] = value[SIDE * k : SIDE * k + SIDE]
        for begin in range(0, width, 128):
            stop = min(begin + 128, width)
            for low, high in TILES:
                result = None
                for y in range(begin // nodes_z, (stop - 1) // nodes_z + 1):
                    node = jnp.clip(lane + (begin - nodes_z * y), 0, nodes_z - 1) + 1
                    sevens = ((node.astype(F32) + 0.5) * (1.0 / DEG)).astype(jnp.int32)
                    got = lane_pick(work_ref[y, low:high], node + sevens)
                    result = got if result is None else jnp.where(lane + begin >= nodes_z * y, got, result)
                out_ref[c, low:high, begin:stop] = result[:, : stop - begin]
        return carry

    lax.fori_loop(0, 3, component, 0)


VM = pl.BlockSpec(memory_space=pltpu.VMEM)
SM = pl.BlockSpec(memory_space=pltpu.SMEM)
FIELD = (3, N, N, ROWS, 128)
MID = (3, N, N - 2, ROWS, 128)
EDGE = (3, N, 2, ROWS, 128)
FACE = (3, 2, N, ROWS, 128)
INNER = (3, N - 2, N, ROWS, 128)


def shape(dims):
    return jax.ShapeDtypeStruct(dims, F32)


def call(kernel, smem, inputs, outs, work=0, rows=FIELD):
    return pl.pallas_call(
        kernel,
        in_specs=[SM] * smem + [VM] * (len(inputs) - smem),
        out_specs=[VM] * len(outs),
        out_shape=[shape(dims) for dims in outs],
        scratch_shapes=[pltpu.VMEM(rows, F32)] * work,
        compiler_params=pltpu.CompilerParams(vmem_limit_bytes=6 << 20),
    )(*inputs)


def swaps(even, odd, axis):
    size = lax.axis_size(axis)
    got_odd = lax.ppermute(odd, axis, [(i, (((i + 1) ^ 1) - 1) % size) for i in range(size)])
    got_even = lax.ppermute(even, axis, [(i, i ^ 1) for i in range(size)])
    return got_even, got_odd


def exchange(ctl, x_faces, fields):
    xe, xo = swaps(*x_faces, "gy")
    ye, yo = call(corner_kernel, 0, (ctl, xe, xo, *fields), (xe.shape, xe.shape))
    ye, yo = swaps(ye, yo, "gx")
    return (xe, xo), (ye, yo)


def from_next(value, axis):
    size = lax.axis_size(axis)
    return lax.ppermute(value, axis, [(i, (i - 1) % size) for i in range(size)])


def local(right_side, guess, material, lame, upper, lower_ratio):
    elems_x, elems_y, elems_z = material.shape
    nodes_y = DEG * elems_y
    w_grad, w_back, w_share = z_matrices(elems_z)
    w_grad = jnp.asarray(w_grad, BF16)
    w_back = jnp.asarray(w_back, BF16)
    w_share = jnp.asarray(w_share, BF16)
    upper_edge = upper[0]
    lower_edge = lower_ratio[0] * upper_edge
    center = (upper_edge + lower_edge) / 2.0
    radius = (upper_edge - lower_edge) / 2.0
    sigma_ratio = center / radius
    pairs = [(jnp.zeros((), F32), 1.0 / center)]
    factor = 1.0 / sigma_ratio
    for step_index in range(CHEB - 1):
        factor_next = 1.0 / (2.0 * sigma_ratio - factor)
        pairs.append((factor_next * factor, 2.0 * factor_next / radius))
        factor = factor_next
    flags = [(lax.axis_index(axis) % 2).astype(F32) for axis in ("gy", "gx")]
    ctl = jnp.stack(flags + [value for pair in pairs for value in pair])
    ctl = jnp.broadcast_to(ctl[:, None, None], (2 + 2 * CHEB, ROWS, 128))
    grid = (N, N, ROWS, 128)
    weight_z = jnp.asarray(np.tile(WEIGHTS, (ROWS, elems_z)), F32)
    coeffs = call(coeff_kernel, 1, (lame, ctl, material, weight_z), (grid,) * 4)
    coeffs = [coeffs[:2], coeffs[2:]]

    plane = (3, N, SIDE, 128)
    staged = (nodes_y + 1, nodes_y + SIDE, 128)
    loads = [call(load_kernel, 0, (ctl, value), (FIELD, FIELD, plane, plane), 1, staged) for value in (guess, right_side)]
    x_halo = from_next(jnp.concatenate([load[2] for load in loads], 0), "gy")
    y_halo = jnp.concatenate([load[3] for load in loads], 0)
    (y_halo,) = call(halo_corner_kernel, 0, (x_halo, y_halo), (y_halo.shape,))
    y_halo = from_next(y_halo, "gx")
    ratio_z = jnp.asarray(np.tile(RATIO, (ROWS, elems_z)), F32)
    ratio_i = jnp.asarray(np.broadcast_to(RATIO[:, None, None], (N, ROWS, 128)), F32)
    weights = (w_grad, w_back, w_share)
    work = (FIELD,) * 3
    both_faces = ((6, N, SIDE, 128),) * 2
    diag = tuple(call(diag_kernel, 0, (*coeffs[tile], ratio_i, ratio_z, w_share), (FIELD,))[0] for tile in range(2))
    got = call(first_mid_kernel, 0, (w_grad, x_halo, *loads[0][:2]), (MID, MID, MID, FIELD) * 2)
    u_mid = [got[0], got[4]]

    def first(tile, extra, outs, scratch):
        inputs = (ctl, *weights, *coeffs[tile], loads[0][tile], x_halo, y_halo, *got[4 * tile + 1 : 4 * tile + 4], *extra)
        return call(lambda *refs: first_kernel(tile, *refs), 0, inputs, (EDGE,) + outs, scratch)

    edge_0, face, *rest = first(0, diag[:1], (FACE, *both_faces, *work), 0)
    x_faces, work_0 = rest[:2], rest[2:]
    edge_1, inner, au = first(1, work_0, (INNER, FIELD), 3)
    u_edge = [edge_0, edge_1]
    b = call(halo_kernel, 0, (x_halo, y_halo, *loads[1][:2]), (FIELD, FIELD))
    change_mid = [None, None]
    change_edge = [None, None]
    inv_mid = [None, None]
    inv_edge = [None, None]
    for count in range(SWEEPS * CHEB):
        stage = count % CHEB
        with_diag = count == 0
        sums = (face, inner, au)
        x_got, y_got = exchange(ctl, x_faces, sums + (diag if with_diag else ()))
        keep_inv = 1 if with_diag else 0

        inputs = (ctl, w_grad, *sums, *x_got) + (diag if with_diag else ())
        for tile in range(2):
            inputs += (u_mid[tile], b[tile]) + (() if with_diag else (inv_mid[tile],))
            inputs += (change_mid[tile],) if stage else ()
        keep_change = 1 if stage < CHEB - 1 else 0
        each = 4 + keep_change + keep_inv
        outs = ((MID, MID, MID, FIELD) + (MID,) * (keep_change + keep_inv)) * 2
        results = call(lambda *refs: mid_kernel(stage, with_diag, *refs), 0, inputs, outs)
        slopes = [None, None]
        for tile in range(2):
            got = results[each * tile : each * (tile + 1)]
            u_mid[tile] = got[0]
            slopes[tile] = got[1:4]
            if keep_change:
                change_mid[tile] = got[4]
            if with_diag:
                inv_mid[tile] = got[-1]

        for tile in range(2):
            inputs = (ctl, *weights, *coeffs[tile], *sums, *x_got, *y_got) + (diag if with_diag else ())
            inputs += (*slopes[tile], u_edge[tile], b[tile])
            inputs += () if with_diag else (inv_edge[tile],)
            inputs += (change_edge[tile],) if stage else ()
            inputs += tuple(work_0) if tile else ()
            outs = (EDGE,) * (1 + keep_change + keep_inv)
            outs += (INNER, FIELD) if tile else (FACE, *((3, N, SIDE, 128),) * 2, *work)
            results = list(
                call(lambda *refs: edge_kernel(tile, stage, with_diag, *refs), 0, inputs, outs, 3 if tile else 0)
            )
            u_edge[tile] = results.pop(0)
            if keep_change:
                change_edge[tile] = results.pop(0)
            if with_diag:
                inv_edge[tile] = results.pop(0)
            if tile:
                inner, au = results
            else:
                face, x_faces, work_0 = results[0], results[1:3], results[3:]
    sums = (face, inner, au)
    x_got, y_got = exchange(ctl, x_faces, sums)

    def store(with_residual, inputs):
        return call(lambda *refs: store_kernel(with_residual, *refs), 0, inputs, (guess.shape,), 1, staged)[0]

    smoothed = store(False, (u_mid[0], u_edge[0], u_mid[1], u_edge[1]))
    return (smoothed, store(True, (ctl, *b, *sums, *x_got, *y_got)))


def solution(mesh):
    placed = (P(None, "gx", "gy"), P(None, "gx", "gy"), P("gx", "gy", None), P(), P(), P())
    return jax.shard_map(
        local,
        mesh=mesh,
        in_specs=placed,
        out_specs=(P(None, "gx", "gy"), P(None, "gx", "gy")),
        check_vma=False,
    )
```

```python
import jax
import jax.numpy as jnp
import numpy as np
from jax import lax
from jax.experimental import pallas as pl
from jax.experimental.pallas import tpu as pltpu
from jax.sharding import PartitionSpec as P

DEG = 7
N = DEG + 1
SWEEPS = 2
CHEB = 3
F32 = jnp.float32
BF16 = jnp.bfloat16
highest = lax.Precision.HIGHEST


def legendre_pair(points, degree):
    prev_poly = points * 0.0 + 1.0
    this_poly = points * 1.0
    for order in range(2, degree + 1):
        next_poly = ((2 * order - 1) * points * this_poly - (order - 1) * prev_poly) / order
        prev_poly = this_poly
        this_poly = next_poly
    return (this_poly, prev_poly)


def gll_tables(degree):
    count = degree + 1
    points = -np.cos(np.pi * np.arange(count) / degree)
    for newton_step in range(60):
        this_poly, prev_poly = legendre_pair(points, degree)
        points = points - (points * this_poly - prev_poly) / (count * this_poly)
    values, unused_poly = legendre_pair(points, degree)
    weights = 2.0 / (degree * (degree + 1) * values**2)
    identity_np = np.eye(count)
    spacing = points[:, None] - points[None, :] + identity_np
    derivative = values[:, None] / (values[None, :] * spacing) * (1.0 - identity_np)
    derivative[0, 0] = -degree * (degree + 1) / 4.0
    derivative[degree, degree] = degree * (degree + 1) / 4.0
    stiff_ratio = (weights[:, None] * derivative**2).sum(0) / weights
    return (weights, derivative, stiff_ratio)


WEIGHTS, DERIV, RATIO = gll_tables(DEG)


def halves(matrix):
    high = matrix.astype(BF16).astype(np.float32)
    low = matrix.astype(np.float32) - high
    return high, low


def z_matrices(blocks):
    width = blocks * N
    node = np.array([DEG * f + k for f in range(blocks) for k in range(N)])
    free = (node > 0) & (node < DEG * blocks)
    share = ((node[:, None] == node[None, :]) & free[:, None] & free[None, :]).astype(np.float64)
    grad = np.kron(np.eye(blocks), DERIV.T)
    back = np.kron(np.eye(blocks), DERIV) @ share
    zero = np.zeros((width, width))
    grad_hi, grad_lo = halves(grad)
    back_hi, back_lo = halves(back)
    w_grad = np.block([[grad_hi, grad_lo], [grad_hi, zero]])
    w_back = np.block([[back_hi, back_lo], [back_hi, zero]])
    w_share = np.concatenate([share, share], 0)
    return w_grad, w_back, w_share


def line_sums(vals, matrix, pairs=range(N // 2)):
    even = [vals[i] + vals[DEG - i] for i in range(N // 2)]
    odd = [vals[i] - vals[DEG - i] for i in range(N // 2)]
    outs = [None] * N
    for p in pairs:
        from_even = None
        from_odd = None
        for i in range(N // 2):
            te = float(np.float32((matrix[p, i] + matrix[p, DEG - i]) / 2.0)) * even[i]
            to = float(np.float32((matrix[p, i] - matrix[p, DEG - i]) / 2.0)) * odd[i]
            from_even = te if from_even is None else from_even + te
            from_odd = to if from_odd is None else from_odd + to
        outs[p] = from_odd + from_even
        outs[DEG - p] = from_odd - from_even
    return outs


def pair_terms(low, high, matrix, i, p):
    even = float(np.float32((matrix[p, i] + matrix[p, DEG - i]) / 2.0)) * (low + high)
    odd = float(np.float32((matrix[p, i] - matrix[p, DEG - i]) / 2.0)) * (low - high)
    return even, odd


def inner_sums(vals, matrix):
    outs = [None] * N
    for p in range(N // 2):
        terms = [pair_terms(vals[i - 1], vals[DEG - i - 1], matrix, i, p) for i in range(1, N // 2)]
        from_even = terms[0][0] + terms[1][0] + terms[2][0]
        from_odd = terms[0][1] + terms[1][1] + terms[2][1]
        outs[p] = from_odd + from_even
        outs[DEG - p] = from_odd - from_even
    return outs


def add_ends(partial, low, high, matrix):
    outs = [None] * N
    for p in range(N // 2):
        from_even, from_odd = pair_terms(low, high, matrix, 0, p)
        outs[p] = partial[p] + (from_odd + from_even)
        outs[DEG - p] = partial[DEG - p] + (from_odd - from_even)
    return outs


def split_pair(value):
    high = value.astype(BF16)
    low = (value - high.astype(F32)).astype(BF16)
    return jnp.concatenate([high, low], axis=-1)


def dot(a, b):
    return jnp.dot(a, b, preferred_element_type=F32)


ROWS = 8
SIDE = 4
ORDER = (0, 3, 1, 2)
UNROLL = 2


def flip(value):
    return jnp.concatenate([value[SIDE:], value[:SIDE]], 0)


def whole(ref):
    return lambda c, i, j: ref[c, i, j]


def by_i(face_ref, inner_ref):
    return lambda c, i, j: face_ref[c, i // DEG, j] if i in (0, DEG) else inner_ref[c, i - 1, j]


def by_j(mid_ref, edge_ref):
    return lambda c, i, j: edge_ref[c, i, j // DEG] if j in (0, DEG) else mid_ref[c, i, j - 1]


def mixed(mid, full):
    return lambda c, i, j: full[c, i, j] if j in (0, DEG) else mid[c, i, j - 1]


def with_halo(src, xr_ref, yr_ref, face_at, c, i, j, tile):
    value = src[c, i, j]
    row = lax.broadcasted_iota(jnp.int32, (ROWS, 128), 0)
    if tile == 0 and i == DEG:
        face = xr_ref[face_at, j]
        value = jnp.where(row < SIDE, value, jnp.concatenate([face, face], 0))
    if isinstance(j, int) and j == DEG:
        face = yr_ref[face_at, i]
        first = jnp.broadcast_to(face[2 * tile : 2 * tile + 1], (ROWS, 128))
        second = jnp.broadcast_to(face[2 * tile + 1 : 2 * tile + 2], (ROWS, 128))
        value = jnp.where(row == SIDE - 1, first, jnp.where(row == ROWS - 1, second, value))
    return value


def received(ctl_ref, axis, even_ref, odd_ref, *at):
    is_even = ctl_ref[axis][:SIDE] < 0.5
    even = even_ref[at]
    odd = odd_ref[at]
    return jnp.where(is_even, even, odd), jnp.where(is_even, odd, even)


def sum_x(ctl_ref, xe_ref, xo_ref, parts, c, face_at, i, j, tile):
    total = parts[tile](c, i, j)
    if 0 < i < DEG:
        return total
    row = lax.broadcasted_iota(jnp.int32, (ROWS, 128), 0)
    across = DEG - i
    if tile == 0:
        right, left = received(ctl_ref, 0, xe_ref, xo_ref, face_at, j)
        face = right if i else left
        face = jnp.concatenate([face, face], 0)
        inner = parts[1](c, across, j)
        low, high = (inner, face) if i else (face, inner)
    else:
        middle = flip(parts[1](c, across, j))
        outer = parts[0](c, across, j)
        low, high = (middle, outer) if i else (outer, middle)
    return total + jnp.where(row < SIDE, low, high)


def sum_all(ctl_ref, faces, parts, c, face_at, i, j, tile):
    xe, xo, ye, yo = faces
    total = sum_x(ctl_ref, xe, xo, parts, c, face_at, i, j, tile)
    if isinstance(j, int) and j in (0, DEG):
        row = lax.broadcasted_iota(jnp.int32, (ROWS, 128), 0)
        top, bottom = received(ctl_ref, 1, ye, yo, face_at, i)
        face = top if j else bottom
        at = SIDE - 1 if j else 0
        first = jnp.broadcast_to(face[2 * tile : 2 * tile + 1], (ROWS, 128))
        second = jnp.broadcast_to(face[2 * tile + 1 : 2 * tile + 2], (ROWS, 128))
        total = total + jnp.where(row == at, first, jnp.where(row == SIDE + at, second, 0.0))
    return total


def loop(count, body, unroll=UNROLL):
    def inner(i, carry):
        body(i)
        return carry

    lax.fori_loop(0, count, inner, 0, unroll=unroll)


def gradients(planes, at, wg_ref, gx_ref, gz_ref):
    flat = jnp.concatenate([planes[c][i] for c in range(3) for i in range(N)], 0)
    both = dot(split_pair(flat), wg_ref[...])
    for c in range(3):
        outs = line_sums(planes[c], DERIV)
        for i in range(N):
            gx_ref[c, i, at] = outs[i]
    both = (both[:, :128] + both[:, 128:]).reshape(3, N, ROWS, 128)
    for c in range(3):
        for i in range(N):
            gz_ref[c, i, at] = both[c, i]


def inner_slopes(u_ref, gy_ref):
    def plane(i):
        for c in range(3):
            outs = inner_sums([u_ref[c, i, at] for at in range(N - 2)], DERIV)
            for j in range(N):
                gy_ref[c, i, j] = outs[j]

    loop(N, plane)


def back_yz(sy, sz, i, wb_ref, fz_ref, fy_ref):
    flat = jnp.concatenate([sz[c][j] for c in range(3) for j in range(N)], 0)
    both = dot(split_pair(flat), wb_ref[...])
    for c in range(3):
        outs = line_sums(sy[c], DERIV.T)
        for j in range(N):
            fy_ref[c, i, j] = outs[j]
    both = (both[:, :128] + both[:, 128:]).reshape(3, N, ROWS, 128)
    for c in range(3):
        fz_ref[c, i] = both[c]


def stress(tile, edge_ref, gy_ref, gx_at, gz_at, lam_ref, mu_ref, wb_ref, sx_ref, fz_ref, fy_ref):
    def plane(i, later=False):
        gy = [
            add_ends([gy_ref[c, i, j] for j in range(N)], edge_ref[c, i, 0], edge_ref[c, i, 1], DERIV)
            for c in range(3)
        ]
        sy = [[None] * N for c in range(3)]
        sz = [[None] * N for c in range(3)]
        for j in range(N):
            gx = [gx_at(c, i, j) for c in range(3)]
            gz = [gz_at(c, i, j) for c in range(3)]
            mu = mu_ref[i, j]
            mu2 = mu + mu
            trace = lam_ref[i, j] * (gx[0] + gy[1][j] + gz[2])
            sxy = mu * (gx[1] + gy[0][j])
            sxz = mu * (gx[2] + gz[0])
            syz = mu * (gy[2][j] + gz[1])
            sx_ref[0, i, j] = mu2 * gx[0] + trace
            sx_ref[1, i, j] = sxy
            sx_ref[2, i, j] = sxz
            sz[0][j] = sxz
            sz[1][j] = syz
            sz[2][j] = mu2 * gz[2] + trace
            sy[0][j] = sxy
            sy[1][j] = mu2 * gy[1][j] + trace
            sy[2][j] = syz
            if later:
                fy_ref[1, i, j] = sy[1][j]
                fy_ref[2, i, j] = syz
                fz_ref[2, i, j] = sz[2][j]
        if not later:
            back_yz(sy, sz, i, wb_ref, fz_ref, fy_ref)

    if tile:
        loop(N, plane)
    else:
        plane(0)
        plane(DEG)
        loop(N - 2, lambda at: plane(at + 1, True))


def late_back(wb_ref, work_0, fz_ref, fy_ref):
    sx_ref, sz_ref, sy_ref = work_0

    def plane(at):
        i = at + 1
        sxy = [sx_ref[1, i, j] for j in range(N)]
        sxz = [sx_ref[2, i, j] for j in range(N)]
        syy = [sy_ref[1, i, j] for j in range(N)]
        syz = [sy_ref[2, i, j] for j in range(N)]
        szz = [sz_ref[2, i, j] for j in range(N)]
        back_yz((sxy, syy, syz), (sxz, syz, szz), i, wb_ref, fz_ref, fy_ref)

    loop(N - 2, plane)


def back(ws_ref, work, out_ref, nodes, planes):
    sx_ref, fz_ref, fy_ref = work
    pairs = sorted({min(i, DEG - i) for i in nodes})
    flat = []
    for j in planes:
        for c in range(3):
            outs = line_sums([sx_ref[c, i, j] for i in range(N)], DERIV.T, pairs)
            flat += [outs[i] + fy_ref[c, i, j] for i in nodes]
    both = dot(split_pair(jnp.concatenate(flat, 0)), ws_ref[...]).reshape(len(planes), 3, len(nodes), ROWS, 128)
    for at, j in enumerate(planes):
        for c in range(3):
            for k, i in enumerate(nodes):
                out_ref[c, k, j] = both[at, c, k] + fz_ref[c, i, j]


def back_loop(ws_ref, work, out_ref, nodes):
    loop(N, lambda j: back(ws_ref, work, out_ref, nodes, (j,)))


def join_y(part_ref):
    row = lax.broadcasted_iota(jnp.int32, (ROWS, 128), 0)
    near = row % SIDE

    def along(i):
        for c in range(3):
            last = part_ref[c, i, DEG]
            start = part_ref[c, i, 0]
            last = last + jnp.where(near < SIDE - 1, jnp.concatenate([start[1:], start[:1]], 0), 0.0)
            start = jnp.where(near > 0, jnp.concatenate([last[-1:], last[:-1]], 0), start)
            part_ref[c, i, DEG] = last
            part_ref[c, i, 0] = start

    loop(part_ref.shape[1], along)


def give_faces(ctl_ref, part_ref, first, xe_ref, xo_ref):
    is_even = ctl_ref[0][:SIDE] < 0.5
    end = part_ref.shape[1] - 1

    def plane(j):
        for c in range(3):
            right = part_ref[c, end, j][SIDE:]
            left = part_ref[c, 0, j][:SIDE]
            xe_ref[first + c, j] = jnp.where(is_even, right, left)
            xo_ref[first + c, j] = jnp.where(is_even, left, right)

    loop(N, plane)


ENDS = (0, DEG)
INSIDE = tuple(range(1, DEG))
ALL = tuple(range(N))


def send_first(ctl_ref, ws_ref, work, face_ref, xe_ref, xo_ref):
    back(ws_ref, work, face_ref, ENDS, ALL)
    join_y(face_ref)
    give_faces(ctl_ref, face_ref, 0, xe_ref, xo_ref)


def finish_second(wb_ref, ws_ref, work, work_0, inner_ref, au_ref):
    back_loop(ws_ref, work, au_ref, ALL)
    join_y(au_ref)
    sx_ref, fz_ref, fy_ref = work
    late_back(wb_ref, work_0, fz_ref, fy_ref)
    back_loop(ws_ref, (work_0[0], fz_ref, fy_ref), inner_ref, INSIDE)
    join_y(inner_ref)


def diag_kernel(lam_ref, mu_ref, ratio_ref, rk_ref, ws_ref, dg_ref):
    def diagonal(i):
        rows = [[None] * N for c in range(3)]
        for j in range(N):
            lam = lam_ref[i, j]
            mu = mu_ref[i, j]
            ri = ratio_ref[i]
            rk = rk_ref[...]
            total = rk + (ri + float(RATIO[j]))
            for c in range(3):
                own = (ri, float(RATIO[j]), rk)[c]
                rows[c][j] = lam * own + mu * (total + own)
        flat = jnp.concatenate([rows[c][j] for c in range(3) for j in range(N)], 0)
        both = dot(split_pair(flat), ws_ref[...]).reshape(3, N, ROWS, 128)
        for c in range(3):
            dg_ref[c, i] = both[c]

    loop(N, diagonal, 1)
    join_y(dg_ref)


def first_mid_kernel(wg_ref, xr_ref, t0_ref, t1_ref, *outs):
    for tile, src in enumerate((t0_ref, t1_ref)):
        u_out, gx_ref, gz_ref, gy_ref = outs[4 * tile : 4 * tile + 4]

        def plane(at):
            planes = [[with_halo(src, xr_ref, None, c, c, i, at + 1, tile) for i in range(N)] for c in range(3)]
            for c in range(3):
                for i in range(N):
                    u_out[c, i, at] = planes[c][i]
            gradients(planes, at, wg_ref, gx_ref, gz_ref)

        loop(N - 2, plane)
        inner_slopes(u_out, gy_ref)


def first_kernel(tile, *refs):
    refs = list(refs)
    take = lambda count: [refs.pop(0) for _ in range(count)]
    ctl_ref, wg_ref, wb_ref, ws_ref, lam_ref, mu_ref, src, xr_ref, yr_ref, gx_ref, gz_ref, gy_ref = take(12)
    if tile == 0:
        (dg_ref,) = take(1)
        u_out, face_ref, xe_ref, xo_ref = take(4)
    else:
        work_0 = take(3)
        u_out, inner_ref, au_ref = take(3)
    work = take(3)
    sx_ref, fz_ref, fy_ref = work
    for k in range(2):
        planes = [[with_halo(src, xr_ref, yr_ref, c, c, i, DEG * k, tile) for i in range(N)] for c in range(3)]
        for c in range(3):
            for i in range(N):
                u_out[c, i, k] = planes[c][i]
        gradients(planes, DEG * k, wg_ref, sx_ref, fz_ref)
    stress(tile, u_out, gy_ref, mixed(gx_ref, sx_ref), mixed(gz_ref, fz_ref), lam_ref, mu_ref, wb_ref, *work)
    if tile == 0:
        send_first(ctl_ref, ws_ref, work, face_ref, xe_ref, xo_ref)
        give_faces(ctl_ref, dg_ref, 3, xe_ref, xo_ref)
    else:
        finish_second(wb_ref, ws_ref, work, work_0, inner_ref, au_ref)


def corner_kernel(ctl_ref, xe_ref, xo_ref, face_ref, inner_ref, au_ref, *refs):
    ye_ref, yo_ref = refs[-2:]
    fields = [(by_i(face_ref, inner_ref), whole(au_ref))]
    if len(refs) > 2:
        fields.append((whole(refs[0]), whole(refs[1])))
    is_even = ctl_ref[1][:SIDE] < 0.5
    for n, parts in enumerate(fields):
        for c in range(3):
            at = 3 * n + c
            for i in range(N):
                rows_t = []
                rows_b = []
                for tile in range(2):
                    top = sum_x(ctl_ref, xe_ref, xo_ref, parts, c, at, i, DEG, tile)
                    bottom = sum_x(ctl_ref, xe_ref, xo_ref, parts, c, at, i, 0, tile)
                    rows_t += [top[SIDE - 1 : SIDE], top[-1:]]
                    rows_b += [bottom[:1], bottom[SIDE : SIDE + 1]]
                top = jnp.concatenate(rows_t, 0)
                bottom = jnp.concatenate(rows_b, 0)
                ye_ref[at, i] = jnp.where(is_even, top, bottom)
                yo_ref[at, i] = jnp.where(is_even, bottom, top)


def invert(diag):
    lane = lax.broadcasted_iota(jnp.int32, (ROWS, 128), 1)
    clamped = (lane == 0) | (lane == 127)
    return jnp.where(clamped, 0.0, 1.0 / jnp.where(clamped, 1.0, diag))


def advance(ctl_ref, stage, u, load, total, inv, change):
    change_new = ctl_ref[3 + 2 * stage] * (inv * (load - total))
    if stage:
        change_new = ctl_ref[2 + 2 * stage] * change + change_new
    return u + change_new, change_new


def mid_kernel(stage, with_diag, *refs):
    refs = list(refs)
    take = lambda count: [refs.pop(0) for _ in range(count)]
    ctl_ref, wg_ref, face_ref, inner_ref, au_ref, xe_ref, xo_ref = take(7)
    parts = (by_i(face_ref, inner_ref), whole(au_ref))
    diag_parts = [whole(ref) for ref in take(2)] if with_diag else None
    ins = []
    for tile in range(2):
        u_ref, b_ref = take(2)
        ins.append((u_ref, b_ref, None if with_diag else take(1)[0], take(1)[0] if stage else None))
    for tile in range(2):
        u_ref, b_ref, inv_ref, change_ref = ins[tile]
        u_out, gx_ref, gz_ref, gy_ref = take(4)
        change_out = take(1 if stage < CHEB - 1 else 0)
        inv_out = take(1)[0] if with_diag else None

        def plane(at):
            j = at + 1
            planes = [[None] * N for c in range(3)]
            for c in range(3):
                for i in range(N):
                    if with_diag:
                        inv = invert(sum_x(ctl_ref, xe_ref, xo_ref, diag_parts, c, 3 + c, i, j, tile))
                        inv_out[c, i, at] = inv
                    else:
                        inv = inv_ref[c, i, at]
                    total = sum_x(ctl_ref, xe_ref, xo_ref, parts, c, c, i, j, tile)
                    change = change_ref[c, i, at] if stage else None
                    planes[c][i], change = advance(ctl_ref, stage, u_ref[c, i, at], b_ref[c, i, j], total, inv, change)
                    if change_out:
                        change_out[0][c, i, at] = change
                    u_out[c, i, at] = planes[c][i]
            gradients(planes, at, wg_ref, gx_ref, gz_ref)

        loop(N - 2, plane)
        inner_slopes(u_out, gy_ref)


def edge_kernel(tile, stage, with_diag, *refs):
    refs = list(refs)
    take = lambda count: [refs.pop(0) for _ in range(count)]
    ctl_ref, wg_ref, wb_ref, ws_ref, lam_ref, mu_ref, face_in, inner_in, au_in = take(9)
    faces = take(4)
    parts = (by_i(face_in, inner_in), whole(au_in))
    diag_parts = [whole(ref) for ref in take(2)] if with_diag else None
    gx_ref, gz_ref, gy_ref, u_ref, b_ref = take(5)
    inv_ref = None if with_diag else take(1)[0]
    change_ref = take(1)[0] if stage else None
    work_0 = take(3) if tile else None
    (u_out,) = take(1)
    change_out = take(1 if stage < CHEB - 1 else 0)
    inv_out = take(1)[0] if with_diag else None
    outs = take(2 if tile else 3)
    work = take(3)
    sx_ref, fz_ref, fy_ref = work
    for k in range(2):
        j = DEG * k
        planes = [[None] * N for c in range(3)]
        for c in range(3):
            for i in range(N):
                if with_diag:
                    inv = invert(sum_all(ctl_ref, faces, diag_parts, c, 3 + c, i, j, tile))
                    inv_out[c, i, k] = inv
                else:
                    inv = inv_ref[c, i, k]
                total = sum_all(ctl_ref, faces, parts, c, c, i, j, tile)
                change = change_ref[c, i, k] if stage else None
                planes[c][i], change = advance(ctl_ref, stage, u_ref[c, i, k], b_ref[c, i, j], total, inv, change)
                if change_out:
                    change_out[0][c, i, k] = change
                u_out[c, i, k] = planes[c][i]
        gradients(planes, j, wg_ref, sx_ref, fz_ref)

    stress(tile, u_out, gy_ref, mixed(gx_ref, sx_ref), mixed(gz_ref, fz_ref), lam_ref, mu_ref, wb_ref, *work)
    if tile == 0:
        send_first(ctl_ref, ws_ref, work, *outs)
    else:
        finish_second(wb_ref, ws_ref, work, work_0, *outs)


def lane_pick(value, index):
    return jnp.take_along_axis(value, index, axis=1, mode="promise_in_bounds")


TILES = ((0, 8), (8, 16), (16, 24), (20, 28))


def plane_kernel(nodes_z, buf_ref, xl_ref, work_ref):
    lane = lax.broadcasted_iota(jnp.int32, (ROWS, 128), 1)
    node = DEG * (lane // N) + lane % N - 1
    free = (node >= 0) & (node < nodes_z)
    node = jnp.clip(node, 0, nodes_z - 1)
    for n in range(2):
        for c in range(3):
            at = 3 * n + c
            work_ref[at, pl.ds(24, 8)] = jnp.zeros((ROWS, 128), F32)
            for low, high in TILES:
                work_ref[at, low:high] = jnp.where(free, lane_pick(buf_ref[n, c, low:high], node), 0.0)
            for j in range(N):
                xl_ref[3 * n + (1, 0, 2)[c], j] = work_ref[at, pl.ds(j, SIDE, stride=DEG)]


def load_kernel(ctl_ref, in_ref, t0_ref, t1_ref, yb_ref, work_ref):
    nodes_x, width = in_ref.shape[1], in_ref.shape[2]
    nodes_z = width // nodes_x
    outs = (t0_ref, t1_ref)
    lane = lax.broadcasted_iota(jnp.int32, (ROWS, 128), 1)
    node = DEG * (lane // N) + lane % N - 1
    free = (node >= 0) & (node < nodes_z)
    node = jnp.clip(node, 0, nodes_z - 1)
    zero = jnp.zeros((ROWS, 128), F32)
    for r in range(4):
        work_ref[nodes_x, pl.ds(8 * r, 8)] = zero

    def component(c, carry):
        for y in range(nodes_x):
            tile, shift = divmod(nodes_z * y, 128)
            at = node + shift
            begin = 128 * tile
            work_ref[y, pl.ds(24, 8)] = zero
            for low, high in TILES:
                here = in_ref[c, low:high, begin : begin + 128]
                got = lane_pick(here, at & 127)
                if shift + nodes_z > 128:
                    stop = min(begin + 256, width)
                    there = in_ref[c, low:high, begin + 128 : stop]
                    if stop < begin + 256:
                        there = jnp.concatenate([there, jnp.zeros((ROWS, begin + 256 - stop), F32)], 1)
                    got = jnp.where(at < 128, got, lane_pick(there, at & 127))
                work_ref[y, low:high] = jnp.where(free, got, 0.0)
        out_c = jnp.where(c == 2, 2, 1 - c)
        for i in range(N):
            for j in range(N):
                for which in range(2):
                    rows = [work_ref[DEG * ORDER[2 * which + k] + i, pl.ds(j, SIDE, stride=DEG)] for k in range(2)]
                    value = jnp.concatenate(rows, 0)
                    outs[which][out_c, i, j] = value
                    if j == 0:
                        yb_ref[out_c, i, pl.ds(2 * which, 1)] = value[:1]
                        yb_ref[out_c, i, pl.ds(2 * which + 1, 1)] = value[SIDE : SIDE + 1]
        return carry

    lax.fori_loop(0, 3, component, 0)


def coeff_kernel(lame_ref, ctl_ref, material_ref, wz_ref, *outs):
    lane = lax.broadcasted_iota(jnp.int32, (ROWS, 128), 1)
    weight_z = wz_ref[...]
    for which in range(2):
        rows = [material_ref[b, ORDER[2 * which + k]][None] for k in range(2) for b in range(SIDE)]
        kind = jnp.concatenate(rows, 0).astype(F32)
        kind = jnp.concatenate([kind, jnp.zeros((ROWS, 128 - kind.shape[1]), F32)], 1)
        kind = lane_pick(kind, lane // N)
        for part in range(2):
            value = jnp.zeros((ROWS, 128), F32)
            for label in range(lame_ref.shape[1]):
                value = jnp.where(kind == float(label), lame_ref[part, label], value)
            value = value * weight_z
            for i in range(N):
                for j in range(N):
                    outs[2 * which + part][i, j] = value * float(WEIGHTS[i] * WEIGHTS[j])


def halo_corner_kernel(xr_ref, yb_ref, out_ref):
    row = lax.broadcasted_iota(jnp.int32, (SIDE, 128), 0)
    for n in range(6):
        for i in range(N):
            value = yb_ref[n, i]
            if i == DEG:
                value = jnp.where(row == 1, jnp.broadcast_to(xr_ref[n, 0][:1], (SIDE, 128)), value)
            out_ref[n, i] = value


def halo_kernel(xr_ref, yr_ref, t0_ref, t1_ref, o0_ref, o1_ref):
    for tile, (src, dst) in enumerate(((t0_ref, o0_ref), (t1_ref, o1_ref))):

        def plane(j):
            for c in range(3):
                for i in range(N):
                    dst[c, i, j] = with_halo(src, xr_ref, yr_ref, 3 + c, c, i, j, tile)

        plane(0)
        loop(N - 2, lambda at: plane(at + 1), 1)
        plane(DEG)


def store_kernel(with_residual, *refs):
    refs = list(refs)
    take = lambda count: [refs.pop(0) for _ in range(count)]
    if with_residual:
        ctl_ref, b0_ref, b1_ref, face_ref, inner_ref, au_ref = take(6)
        faces = take(4)
        sums = (by_i(face_ref, inner_ref), whole(au_ref))
        loads = (whole(b0_ref), whole(b1_ref))
        parts = [
            lambda c, i, j, tile=tile: loads[tile](c, i, j) - sum_all(ctl_ref, faces, sums, c, c, i, j, tile)
            for tile in range(2)
        ]
    else:
        parts = [by_j(*take(2)) for tile in range(2)]
    out_ref, work_ref = refs
    nodes_x, width = out_ref.shape[1], out_ref.shape[2]
    nodes_z = width // nodes_x
    lane = lax.broadcasted_iota(jnp.int32, (ROWS, 128), 1)

    def component(c, carry):
        in_c = jnp.where(c == 2, 2, 1 - c)
        for i in range(DEG):
            for j in range(DEG):
                for which in range(2):
                    value = parts[which](in_c, i, j)
                    for k in range(2):
                        at = DEG * ORDER[2 * which + k] + i
                        work_ref[at, pl.ds(j, SIDE, stride=DEG)] = value[SIDE * k : SIDE * k + SIDE]
        for begin in range(0, width, 128):
            stop = min(begin + 128, width)
            for low, high in TILES:
                result = None
                for y in range(begin // nodes_z, (stop - 1) // nodes_z + 1):
                    node = jnp.clip(lane + (begin - nodes_z * y), 0, nodes_z - 1) + 1
                    sevens = ((node.astype(F32) + 0.5) * (1.0 / DEG)).astype(jnp.int32)
                    got = lane_pick(work_ref[y, low:high], node + sevens)
                    result = got if result is None else jnp.where(lane + begin >= nodes_z * y, got, result)
                out_ref[c, low:high, begin:stop] = result[:, : stop - begin]
        return carry

    lax.fori_loop(0, 3, component, 0)


VM = pl.BlockSpec(memory_space=pltpu.VMEM)
SM = pl.BlockSpec(memory_space=pltpu.SMEM)
FIELD = (3, N, N, ROWS, 128)
MID = (3, N, N - 2, ROWS, 128)
EDGE = (3, N, 2, ROWS, 128)
FACE = (3, 2, N, ROWS, 128)
INNER = (3, N - 2, N, ROWS, 128)


def shape(dims):
    return jax.ShapeDtypeStruct(dims, F32)


def call(kernel, smem, inputs, outs, work=0, rows=FIELD):
    return pl.pallas_call(
        kernel,
        in_specs=[SM] * smem + [VM] * (len(inputs) - smem),
        out_specs=[VM] * len(outs),
        out_shape=[shape(dims) for dims in outs],
        scratch_shapes=[pltpu.VMEM(rows, F32)] * work,
        compiler_params=pltpu.CompilerParams(vmem_limit_bytes=6 << 20),
    )(*inputs)


def swaps(even, odd, axis):
    size = lax.axis_size(axis)
    got_odd = lax.ppermute(odd, axis, [(i, (((i + 1) ^ 1) - 1) % size) for i in range(size)])
    got_even = lax.ppermute(even, axis, [(i, i ^ 1) for i in range(size)])
    return got_even, got_odd


def exchange(ctl, x_faces, fields):
    xe, xo = swaps(*x_faces, "gy")
    ye, yo = call(corner_kernel, 0, (ctl, xe, xo, *fields), (xe.shape, xe.shape))
    ye, yo = swaps(ye, yo, "gx")
    return (xe, xo), (ye, yo)


def from_next(value, axis):
    size = lax.axis_size(axis)
    return lax.ppermute(value, axis, [(i, (i - 1) % size) for i in range(size)])


def local(right_side, guess, material, lame, upper, lower_ratio):
    elems_x, elems_y, elems_z = material.shape
    nodes_y = DEG * elems_y
    w_grad, w_back, w_share = z_matrices(elems_z)
    w_grad = jnp.asarray(w_grad, BF16)
    w_back = jnp.asarray(w_back, BF16)
    w_share = jnp.asarray(w_share, BF16)
    upper_edge = upper[0]
    lower_edge = lower_ratio[0] * upper_edge
    center = (upper_edge + lower_edge) / 2.0
    radius = (upper_edge - lower_edge) / 2.0
    sigma_ratio = center / radius
    pairs = [(jnp.zeros((), F32), 1.0 / center)]
    factor = 1.0 / sigma_ratio
    for step_index in range(CHEB - 1):
        factor_next = 1.0 / (2.0 * sigma_ratio - factor)
        pairs.append((factor_next * factor, 2.0 * factor_next / radius))
        factor = factor_next
    flags = [(lax.axis_index(axis) % 2).astype(F32) for axis in ("gy", "gx")]
    ctl = jnp.stack(flags + [value for pair in pairs for value in pair])
    ctl = jnp.broadcast_to(ctl[:, None, None], (2 + 2 * CHEB, ROWS, 128))
    grid = (N, N, ROWS, 128)
    weight_z = jnp.asarray(np.tile(WEIGHTS, (ROWS, elems_z)), F32)
    coeffs = call(coeff_kernel, 1, (lame, ctl, material, weight_z), (grid,) * 4)
    coeffs = [coeffs[:2], coeffs[2:]]

    corner = jnp.stack([guess[:, :, :128], right_side[:, :, :128]])
    nodes_z = DEG * elems_z - 1
    (first_plane,) = call(
        lambda *refs: plane_kernel(nodes_z, *refs), 0, (corner,), ((6, N, SIDE, 128),), 1, (6, nodes_y + SIDE, 128)
    )
    x_halo = from_next(first_plane, "gy")
    plane = (3, N, SIDE, 128)
    staged = (nodes_y + 1, nodes_y + SIDE, 128)
    loads = [call(load_kernel, 0, (ctl, value), (FIELD, FIELD, plane), 1, staged) for value in (guess, right_side)]
    y_halo = jnp.concatenate([load[2] for load in loads], 0)
    (y_halo,) = call(halo_corner_kernel, 0, (x_halo, y_halo), (y_halo.shape,))
    y_halo = from_next(y_halo, "gx")
    ratio_z = jnp.asarray(np.tile(RATIO, (ROWS, elems_z)), F32)
    ratio_i = jnp.asarray(np.broadcast_to(RATIO[:, None, None], (N, ROWS, 128)), F32)
    weights = (w_grad, w_back, w_share)
    work = (FIELD,) * 3
    both_faces = ((6, N, SIDE, 128),) * 2
    diag = tuple(call(diag_kernel, 0, (*coeffs[tile], ratio_i, ratio_z, w_share), (FIELD,))[0] for tile in range(2))
    got = call(first_mid_kernel, 0, (w_grad, x_halo, *loads[0][:2]), (MID, MID, MID, FIELD) * 2)
    u_mid = [got[0], got[4]]

    def first(tile, extra, outs, scratch):
        inputs = (ctl, *weights, *coeffs[tile], loads[0][tile], x_halo, y_halo, *got[4 * tile + 1 : 4 * tile + 4], *extra)
        return call(lambda *refs: first_kernel(tile, *refs), 0, inputs, (EDGE,) + outs, scratch)

    edge_0, face, *rest = first(0, diag[:1], (FACE, *both_faces, *work), 0)
    x_faces, work_0 = rest[:2], rest[2:]
    edge_1, inner, au = first(1, work_0, (INNER, FIELD), 3)
    u_edge = [edge_0, edge_1]
    b = call(halo_kernel, 0, (x_halo, y_halo, *loads[1][:2]), (FIELD, FIELD))
    change_mid = [None, None]
    change_edge = [None, None]
    inv_mid = [None, None]
    inv_edge = [None, None]
    for count in range(SWEEPS * CHEB):
        stage = count % CHEB
        with_diag = count == 0
        sums = (face, inner, au)
        x_got, y_got = exchange(ctl, x_faces, sums + (diag if with_diag else ()))
        keep_inv = 1 if with_diag else 0

        inputs = (ctl, w_grad, *sums, *x_got) + (diag if with_diag else ())
        for tile in range(2):
            inputs += (u_mid[tile], b[tile]) + (() if with_diag else (inv_mid[tile],))
            inputs += (change_mid[tile],) if stage else ()
        keep_change = 1 if stage < CHEB - 1 else 0
        each = 4 + keep_change + keep_inv
        outs = ((MID, MID, MID, FIELD) + (MID,) * (keep_change + keep_inv)) * 2
        results = call(lambda *refs: mid_kernel(stage, with_diag, *refs), 0, inputs, outs)
        slopes = [None, None]
        for tile in range(2):
            got = results[each * tile : each * (tile + 1)]
            u_mid[tile] = got[0]
            slopes[tile] = got[1:4]
            if keep_change:
                change_mid[tile] = got[4]
            if with_diag:
                inv_mid[tile] = got[-1]

        for tile in range(2):
            inputs = (ctl, *weights, *coeffs[tile], *sums, *x_got, *y_got) + (diag if with_diag else ())
            inputs += (*slopes[tile], u_edge[tile], b[tile])
            inputs += () if with_diag else (inv_edge[tile],)
            inputs += (change_edge[tile],) if stage else ()
            inputs += tuple(work_0) if tile else ()
            outs = (EDGE,) * (1 + keep_change + keep_inv)
            outs += (INNER, FIELD) if tile else (FACE, *((3, N, SIDE, 128),) * 2, *work)
            results = list(
                call(lambda *refs: edge_kernel(tile, stage, with_diag, *refs), 0, inputs, outs, 3 if tile else 0)
            )
            u_edge[tile] = results.pop(0)
            if keep_change:
                change_edge[tile] = results.pop(0)
            if with_diag:
                inv_edge[tile] = results.pop(0)
            if tile:
                inner, au = results
            else:
                face, x_faces, work_0 = results[0], results[1:3], results[3:]
    sums = (face, inner, au)
    x_got, y_got = exchange(ctl, x_faces, sums)

    def store(with_residual, inputs):
        return call(lambda *refs: store_kernel(with_residual, *refs), 0, inputs, (guess.shape,), 1, staged)[0]

    smoothed = store(False, (u_mid[0], u_edge[0], u_mid[1], u_edge[1]))
    return (smoothed, store(True, (ctl, *b, *sums, *x_got, *y_got)))


def solution(mesh):
    placed = (P(None, "gx", "gy"), P(None, "gx", "gy"), P("gx", "gy", None), P(), P(), P())
    return jax.shard_map(
        local,
        mesh=mesh,
        in_specs=placed,
        out_specs=(P(None, "gx", "gy"), P(None, "gx", "gy")),
        check_vma=False,
    )
```
